32 devices in a mesh: groups: 2 (over x), tp: 8 (over z, y), blk: 2 (over core).
Axes of the slice: x: 2, y: 2, z: 4, core: 2. Of those that a mesh axis runs over, the one named last changes fastest.
Arguments:
- tokens: bfloat16 [4096, 7168], P(('groups', 'tp')), parts along dimension 0, may hold values from -6 to 6
- gate_weight: bfloat16 [7168, 2048], P('tp', 'blk'), may hold values from -0.0625 to 0.0625
- up_weight: bfloat16 [7168, 2048], P('tp', 'blk'), may hold values from -0.0625 to 0.0625
- down_weight: bfloat16 [2048, 7168], P('blk', 'tp'), may hold values from -0.125 to 0.125
Outputs:
- mixed: bfloat16 [4096, 7168], P(('groups', 'blk'), 'tp'), parts along dimension 0
The draws below stay inside these ranges and needn't reach their ends.
There are 2 independent parts, one for each index of `groups`. The reference program is written for one: setup_inputs(seed, part) draws one part's arguments, and reference() takes and returns one part's arrays. A program takes and returns all parts, laid end to end along the dimension named above; an argument that names none is the same for every part. Nothing has to cross between parts.
All inputs are finite; a program needn't handle non-finite values.
Results may differ from the reference program's by a relative error of at most 0.005.
Values may be sent and summed in bfloat16 or wider, within the bound.
A program may use at most 128 MiB of HBM per device.

```python
import jax
import jax.numpy as jnp

D = 7168
FF = 2048
TOKENS = 2048


def shard_levels(key, extent, shards, least, top_value):
    gain, own = 1.0, jax.random.fold_in(key, 6)
    for position, blocks in shards:
        heights = jnp.exp(jax.random.uniform(jax.random.fold_in(own, position), (blocks,), jnp.float32, least / len(shards), top_value / len(shards)))
        gain = gain * jnp.repeat(heights, extent[position] // blocks).reshape([-1 if axis == position else 1 for axis in range(len(extent))])
    return gain


def bell_draw(stream_key, shape, spread, bound, cuts=(), dtype=jnp.bfloat16):
    factor_of = shard_levels(stream_key, shape, cuts, -0.22, 0.18) if cuts else 1.0
    array = jax.random.normal(stream_key, shape, jnp.float32) * spread * factor_of
    return jnp.minimum(jnp.maximum(array, -bound), bound).astype(dtype)


def setup_inputs(seed: int = 0, part: int = 0) -> dict:
    key_list = jax.random.split(jax.random.key(seed), 5)
    own_keys = jax.random.split(jax.random.fold_in(key_list[4], part), 5)
    tokens = bell_draw(own_keys[0], (TOKENS, D), 1.0, 6.0, ((0, 8),))
    gate_weight = bell_draw(key_list[1], (D, FF), D ** -0.5, 0.0625, ((0, 8), (1, 2)))
    up_weight = bell_draw(key_list[2], (D, FF), D ** -0.5, 0.0625, ((0, 8), (1, 2)))
    down_weight = bell_draw(key_list[3], (FF, D), FF ** -0.5, 0.125, ((0, 2), (1, 8)))
    return dict(tokens=tokens, gate_weight=gate_weight, up_weight=up_weight, down_weight=down_weight)


def reference(tokens, gate_weight, up_weight, down_weight):
    gate = jnp.dot(tokens, gate_weight, preferred_element_type=jnp.float32)
    up = jnp.dot(tokens, up_weight, preferred_element_type=jnp.float32)
    hidden = (jax.nn.silu(gate) * up).astype(jnp.bfloat16)
    return jnp.dot(hidden, down_weight, preferred_element_type=jnp.float32).astype(jnp.bfloat16)
```

```python
import functools

import jax
import jax.numpy as jnp
from jax import lax
from jax.experimental import pallas as pl
from jax.experimental.pallas import tpu as pltpu
from jax.sharding import PartitionSpec as P

MESH = pl.DeviceIdType.MESH
ANY = pl.BlockSpec(memory_space=pl.ANY)


def flip1(i):
    return i + 1 - 2 * (i % 2)


def greet(devices):
    barrier = pltpu.get_barrier_semaphore()
    for device in devices:
        pl.semaphore_signal(barrier, inc=1, device_id=device, device_id_type=MESH)
    pl.semaphore_wait(barrier, len(devices))


def flip2(i):
    return i + 2 - 4 * ((i // 2) % 2)


CUT = 8


def layer(
    G, n, B,
    tok, gate, up, down, out,
    T, W, D, both, mine_h, H, total,
    lsem, tok_send, tok_recv, core_send, core_recv,
    w_send, w_recv, x_send, x_recv, d_send, d_recv,
    h_send, h_recv, f_send, f_recv,
):
    g, t, b = lax.axis_index("groups"), lax.axis_index("tp"), lax.axis_index("blk")
    h = n // B
    a, j = t // h, t % h
    half, pairs = h // 2, n // 2
    p, y = t // 2, t % 2
    other = (g, t, 1 - b)
    across = (g, flip1(t), b)
    R, K = tok.shape
    width = K // B
    depth, units = gate.shape[0], gate.shape[1] // h
    part = depth // G
    mine = pl.ds(pl.multiple_of(b * width, 128), width)
    theirs = pl.ds(pl.multiple_of((1 - b) * width, 128), width)
    square = h == 4
    cut = R * CUT // 16
    upper, lower_rows = pl.ds(0, cut), pl.ds(cut, R - cut)

    greet(
        [(g, (t + d) % n, b) for d in range(1, n)]
        + [(g, 2 * ((p + d) % pairs) + y, 1 - b) for d in range(1, pairs)]
        + [((g + e) % G, t, b) for e in range(1, G)]
        + [other]
    )

    def remote(src, dst, send, recv, device):
        return pltpu.make_async_remote_copy(
            src_ref=src, dst_ref=dst, send_sem=send, recv_sem=recv,
            device_id=device, device_id_type=MESH,
        )

    pending = []

    def push(*copy):
        c = remote(*copy)
        c.start()
        pending.append(c)

    def local(src, dst, sem):
        return pltpu.make_async_copy(src, dst, sem)

    def rows_of(i, s):
        if square:
            i = flip1(i) if s % 2 else i
            return flip2(i) if s // 2 else i
        return (i + h - s) % h

    def token_block(s):
        return T.at[rows_of(j, s), :, mine]

    def w_block(source, first, size, k):
        start = pl.multiple_of(source * depth + first, 16)
        return W.at[pl.ds(start, size), pl.ds(k * units, units)]

    own_columns = pl.ds(pl.multiple_of(j * units, 128), units)
    loads = [
        local(gate.at[:, own_columns], w_block(t, 0, depth, 0), lsem.at[0]),
        local(up.at[:, own_columns], w_block(t, 0, depth, 1), lsem.at[1]),
        local(tok, T.at[j], lsem.at[2]),
        local(down, D.at[b], lsem.at[3]),
    ]

    first = g * part
    rows = pl.ds(pl.multiple_of(first, 16), part)
    order = [d for k in range(1, n // 2) for d in (k, n - k)] + [n // 2]
    for d in order:
        dest = (t + d) % n
        cols = pl.ds(pl.multiple_of((dest % h) * units, 128), units)
        for k in range(2):
            push(
                (gate, up)[k].at[rows, cols], w_block(t, first, part, k),
                w_send.at[d, k], w_recv.at[d, k], (g, dest, b),
            )

    for s in (2, 1) if square else range(1, h):
        dest = rows_of(j, s) if square else (j + s) % h
        push(tok.at[:, mine], T.at[j, :, mine], tok_send.at[s], tok_recv.at[s], (g, a * h + dest, b))
    push(down, D.at[b], d_send, d_recv, other)
    for load in loads:
        load.start()

    for d in order:
        source = (t + n - d) % n
        for k in range(2):
            block = w_block(source, first, part, k)
            remote(block, block, w_send.at[d, k], w_recv.at[d, k], other).wait_recv()
            for e in range(1, G):
                push(block, block, x_send.at[e, d, k], x_recv.at[e, d, k], ((g + e) % G, t, b))
    for load in loads:
        load.wait()
    remote(D.at[1 - b], D.at[1 - b], d_send, d_recv, other).wait_recv()
    total[...] = jnp.zeros_like(total)

    def tokens_arrive(s):
        block = token_block(s)
        if square and s == 3:
            for i, r in ((3, upper), (0, lower_rows)):
                piece = T.at[rows_of(j, s), r, mine]
                remote(piece, piece, tok_send.at[i], tok_recv.at[i], other).wait_recv()
        else:
            remote(block, block, tok_send.at[s], tok_recv.at[s], other).wait_recv()
        if square and s < 3:
            piece = T.at[rows_of(j, s), (upper, lower_rows)[s - 1], mine]
            target = flip2(j) if s == 1 else flip1(j)
            i = 3 if s == 1 else 0
            push(piece, piece, tok_send.at[i], tok_recv.at[i], (g, a * h + target, b))

        push(block, block, core_send.at[s], core_recv.at[s], other)

    def compute(s):
        slot = rows_of(j, s)
        if s > 0:
            block = T.at[slot, :, theirs]
            remote(block, block, core_send.at[s], core_recv.at[s], other).wait_recv()
        tiles = 4 if K % 512 == 0 else 1
        tile = K // tiles
        both[...] = jnp.zeros_like(both)

        def body(i, carry):
            k = pl.ds(pl.multiple_of(i * tile, 128), tile)
            both[...] += jnp.dot(T[slot, :, k], W[k, :], preferred_element_type=jnp.float32)
            return carry

        lax.fori_loop(0, tiles, body, 0)
        hidden = (jax.nn.silu(both[:, :units]) * both[:, units:]).astype(out.dtype)
        mine_h[s] = hidden

        @pl.when(a == b)
        def _():
            H[s, j, b] = hidden

        for d in sorted(range(1, pairs), key=lambda d: min(d, pairs - d)):
            push(
                mine_h.at[s], H.at[s, j, b], h_send.at[s, d], h_recv.at[s, j // 2, b],
                (g, 2 * ((p + d) % pairs) + y, a),
            )

        @pl.when(a != b)
        def _():
            remote(mine_h.at[s], H.at[s, j, b], h_send.at[s, 0], h_recv.at[s, j // 2, b], other).start()

    def pass_on(s):
        for k in range(half):
            for c in range(B):
                block = H.at[s, 2 * k + y, c]

                @pl.when(jnp.logical_not((a == b) & (j // 2 == k) & (c == b)))
                def _():
                    remote(block, block, h_send.at[s, 0], h_recv.at[s, k, c], other).wait_recv()

                push(block, block, f_send.at[s, k, c], f_recv.at[s, k, c], across)

    def lower(s):
        for k in range(half):
            for c in range(B):
                block = H.at[s, 2 * k + 1 - y, c]
                remote(block, block, f_send.at[s, k, c], f_recv.at[s, k, c], across).wait_recv()

        def body(i, carry):
            r = rows_of(i, s)
            term = total[r]
            for c in range(B):
                term += jnp.dot(
                    H[s, i, c], D[c, pl.ds(pl.multiple_of(i * units, 128), units), :],
                    preferred_element_type=jnp.float32,
                )
            total[r] = term
            return carry

        lax.fori_loop(0, h, body, 0)

    for d in order:
        source = (t + n - d) % n
        for e in range(1, G):
            for k in range(2):
                block = w_block(source, ((g + G - e) % G) * part, part, k)
                remote(block, block, x_send.at[e, d, k], x_recv.at[e, d, k], other).wait_recv()

    compute(0)
    for s in range(1, h):
        tokens_arrive(s)
        compute(s)
        pass_on(s - 1)
        if s >= 2:
            lower(s - 2)
    pass_on(h - 1)
    lower(h - 2)
    lower(h - 1)
    for r in range(h):
        out[pl.ds(r * R, R), :] = total[r].astype(out.dtype)

    for c in pending:
        c.wait_send()
    @pl.when(a != b)
    def _():
        for s in range(h):
            remote(mine_h.at[s], mine_h.at[s], h_send.at[s, 0], h_recv.at[s, 0, 0], other).wait_send()


def local(G, n, B, tokens, gate_weight, up_weight, down_weight):
    h = n // B
    R, K = tokens.shape
    depth, wide = gate_weight.shape
    units, columns = wide // h, down_weight.shape[1]
    dtype = tokens.dtype
    DMA = pltpu.SemaphoreType.DMA
    return pl.pallas_call(
        functools.partial(layer, G, n, B),
        out_shape=jax.ShapeDtypeStruct((h * R, columns), dtype),
        in_specs=[ANY] * 4,
        out_specs=pl.BlockSpec(memory_space=pltpu.VMEM),
        scratch_shapes=[
            pltpu.VMEM((h, R, K), dtype),
            pltpu.VMEM((K, 2 * units), dtype),
            pltpu.VMEM((B, wide, columns), dtype),
            pltpu.VMEM((R, 2 * units), jnp.float32),
            pltpu.VMEM((h, R, units), dtype),
            pltpu.VMEM((h, h, B, R, units), dtype),
            pltpu.VMEM((h, R, columns), jnp.float32),
            DMA((4,)),
            DMA((h,)), DMA((h,)), DMA((h,)), DMA((h,)),
            DMA((n, 2)), DMA((n, 2)),
            DMA((G, n, 2)), DMA((G, n, 2)),
            DMA, DMA,
            DMA((h, n // 2)), DMA((h, h // 2, B)),
            DMA((h, h // 2, B)), DMA((h, h // 2, B)),
        ],
        compiler_params=pltpu.CompilerParams(
            collective_id=0, has_side_effects=True, vmem_limit_bytes=63_000_000
        ),
        name="layer",
    )(tokens, gate_weight, up_weight, down_weight)


LANES = 128


def column_layer(
    G, n, B,
    tok, gate, up, down, out,
    X, W, D, Q, S, R, S2, R2, hs, H, acc,
    l_w, l_x, l_d,
    w_send, w_recv, x_send, x_recv, t_send, t_recv, c_send, c_recv,
    d_send, d_recv, s_send, s_recv, z_send, z_recv, h_send, h_recv,
    r_send, r_recv, y_send, y_recv,
):
    g, t, b = lax.axis_index("groups"), lax.axis_index("tp"), lax.axis_index("blk")
    h = n // B
    z, y, j, a = t // 2, t % 2, t % h, t // h
    zz = z % 2
    inner = zz + a == 1
    outer = zz + a != 1
    own, foreign = b == a, b != a
    rows, depth, wide = tok.shape[0], gate.shape[0], gate.shape[1]
    part = depth // G
    chunks = wide // LANES
    mirror = 2 * (n // 2 - 1 - z) + y
    other = (g, t, 1 - b)
    beside = (g, flip1(t), b)
    along = flip2(t)
    facing = 2 * (n // 2 - 1 - z) + y

    greet(
        [(g, (t + d) % n, c) for d in range(1, n) for c in range(B)]
        + [other]
        + [((g + e) % G, t, b) for e in range(1, G)]
    )

    def remote(src, dst, send, recv, device):
        return pltpu.make_async_remote_copy(
            src_ref=src, dst_ref=dst, send_sem=send, recv_sem=recv,
            device_id=device, device_id_type=MESH,
        )

    def push(*copy):
        remote(*copy).start()

    def got(ref, sem):
        remote(ref, ref, sem, sem, other).wait_recv()

    def sent(ref, sem):
        remote(ref, ref, sem, sem, other).wait_send()

    def lanes(k):
        return pl.ds(pl.multiple_of(k * LANES, LANES), LANES)

    def slice_of(chip):
        return pl.ds(pl.multiple_of(chip * depth, LANES), depth)

    def mirrored(chip):
        return 2 * (n // 2 - 1 - chip // 2) + chip % 2

    def partner(d):
        i = flip1(j) if d % 2 else j
        return flip2(i) if d // 2 else i

    share = pl.ds(pl.multiple_of(g * part, 16), part)
    landed = pl.ds(pl.multiple_of(depth + g * part, 16), part)

    def w_piece(c, k):
        return W.at[c, landed, pl.ds(k * LANES, LANES)]

    def x_block(i, k):
        return X.at[
            i % 2, pl.ds(pl.multiple_of(i // 2 * rows, 16), rows),
            pl.ds(pl.multiple_of(k * depth, LANES), depth),
        ]

    for c in range(chunks):
        for k in range(2):
            push(
                (gate, up)[k].at[share, lanes(c)], w_piece(c, k),
                w_send.at[c, k], w_recv.at[c, k], (g, mirror, b),
            )
        if c == 0:
            for d in (3, 1, 2):
                chip = a * h + partner(d)
                source = chip + b * (mirrored(chip) - chip)
                push(tok.at[:, slice_of(source)], x_block(j, b), t_send.at[d], t_recv.at[d], (g, chip, b))
    loads = []
    for k, chip in enumerate((t, mirror)):
        loads.append(pltpu.make_async_copy(tok.at[:, slice_of(chip)], x_block(j, k), l_x.at[k]))
    for c in range(chunks):
        for k in range(2):
            loads.append(pltpu.make_async_copy(
                (gate, up)[k].at[:, lanes(c)], W.at[c, pl.ds(0, depth), pl.ds(k * LANES, LANES)], l_w.at[c, k],
            ))
    for load in loads:
        load.start()
    down_loads = []

    def d_block(c, k):
        return D.at[c, pl.ds(pl.multiple_of(k * LANES, LANES), LANES), :]

    for c in range(chunks):
        piece = down.at[pl.ds(c * LANES, LANES), :]
        load = pltpu.make_async_copy(piece, d_block(c, b), l_d.at[c])
        load.start()
        down_loads.append(load)
        push(piece, d_block(c, b), d_send.at[c], d_recv.at[c], other)
    acc[...] = jnp.zeros_like(acc)

    def weights_arrive(c):
        for k in range(2):
            got(w_piece(c, k), w_recv.at[c, k])
        block = W.at[c, landed, :]
        for e in range(1, G):
            push(block, block, x_send.at[e, c], x_recv.at[e, c], ((g + e) % G, t, b))

    def partial_sums(c):
        for e in range(1, G):
            start = pl.multiple_of(depth + (g + G - e) % G * part, 16)
            got(W.at[c, pl.ds(start, part), :], x_recv.at[e, c])
        S[c] = jnp.dot(X[1 - y], W[c], preferred_element_type=jnp.float32).astype(S.dtype)
        push(S.at[c], R.at[c], s_send.at[c], s_recv.at[c], beside)
        Q[c] = jnp.dot(X[y], W[c], preferred_element_type=jnp.float32)

    def hand_over(c):
        got(R.at[c], s_recv.at[c])
        S2[c] = (Q[c] + R[c].astype(jnp.float32)).astype(S2.dtype)
        push(S2.at[c], R2.at[c], z_send.at[c], z_recv.at[c], (g, along, b))

    def h_piece(c, k):
        return H.at[y, c, :, lanes(k)]

    def finish(c):
        got(R.at[c], s_recv.at[c])
        got(R2.at[c], z_recv.at[c])
        both = Q[c] + R[c].astype(jnp.float32) + R2[c].astype(jnp.float32)
        hidden = (jax.nn.silu(both[:, :LANES]) * both[:, LANES:]).astype(hs.dtype)
        hs[c] = hidden
        push(hs.at[c], h_piece(c, b), h_send.at[c, 0], h_recv.at[c, b], (g, facing, a))
        push(hs.at[c], h_piece(c, b), h_send.at[c, 1], h_recv.at[c, b], (g, along, a))

        @pl.when(own)
        def _():
            H[y, c, :, lanes(b)] = hidden

        @pl.when(foreign)
        def _():
            push(hs.at[c], h_piece(c, b), h_send.at[c, 2], h_recv.at[c, b], other)

    def spread(c):
        block = H.at[y, c]

        @pl.when(jnp.logical_and(own, inner))
        def _():
            got(h_piece(c, 1 - b), h_recv.at[c, 1 - b])

        @pl.when(jnp.logical_and(own, outer))
        def _():
            for k in range(B):
                got(h_piece(c, k), h_recv.at[c, k])

        @pl.when(jnp.logical_and(foreign, inner))
        def _():
            for k in range(B):
                got(h_piece(c, k), h_recv.at[c, k])
            push(block, block, r_send.at[c], r_recv.at[c], (g, along, b))

        @pl.when(jnp.logical_and(foreign, outer))
        def _():
            got(block, r_recv.at[c])

        push(block, block, y_send.at[c], y_recv.at[c], beside)

    def project(c):
        got(H.at[1 - y, c], y_recv.at[c])
        for k in range(2):
            acc[k] += jnp.dot(H[k, c], D[c], preferred_element_type=jnp.float32)

    def step(c, role, stage):
        @pl.when(jnp.logical_and(role, jnp.logical_and(c >= 0, c < chunks)))
        def _():
            stage(c)

    weights_arrive(0)
    for load in loads:
        load.wait()
    for d in (1, 2, 3):
        block = x_block(partner(d), b)
        got(block, t_recv.at[d])
        push(block, block, c_send.at[d], c_recv.at[d], other)
    for d in (1, 2, 3):
        got(x_block(partner(d), 1 - b), c_recv.at[d])
    for c in range(chunks):
        down_loads[c].wait()
        got(d_block(c, 1 - b), d_recv.at[c])

    always = n > 0

    def body(i, carry):
        step(i - 3, inner, finish)
        step(i - 2, outer, hand_over)
        step(i - 1, always, partial_sums)
        step(i - 4, own, spread)
        step(i - 5, own, project)
        late = 2 * (i - chunks)
        for k in range(2):
            step(late + k, foreign, spread)
        for k in range(2):
            step(late - 2 + k, foreign, project)
        step(i, always, weights_arrive)
        return carry

    lax.fori_loop(1, chunks + 5, body, 0)

    for i in range(h):
        out[pl.ds(i * rows, rows), :] = acc[i % 2, pl.ds(i // 2 * rows, rows), :].astype(out.dtype)

    for d in (1, 2, 3):
        sent(x_block(j, 0), t_send.at[d])
        sent(x_block(j, 0), c_send.at[d])

    def drain(c, carry):
        for k in range(2):
            sent(w_piece(c, k), w_send.at[c, k])
        for e in range(1, G):
            sent(W.at[c, landed, :], x_send.at[e, c])
        sent(d_block(c, b), d_send.at[c])
        sent(S.at[c], s_send.at[c])
        sent(H.at[y, c], y_send.at[c])

        @pl.when(outer)
        def _():
            sent(S2.at[c], z_send.at[c])

        @pl.when(inner)
        def _():
            sent(hs.at[c], h_send.at[c, 0])
            sent(hs.at[c], h_send.at[c, 1])

        @pl.when(jnp.logical_and(inner, foreign))
        def _():
            sent(hs.at[c], h_send.at[c, 2])
            sent(H.at[y, c], r_send.at[c])

        return carry

    lax.fori_loop(0, chunks, drain, 0)


def column_local(G, n, B, tokens, gate_weight, up_weight, down_weight):
    h = n // B
    rows = tokens.shape[0]
    depth, wide = gate_weight.shape
    columns = down_weight.shape[1]
    chunks = wide // LANES
    half = h // 2 * rows
    dtype = tokens.dtype
    DMA = pltpu.SemaphoreType.DMA
    pair = pltpu.VMEM((chunks, half, 2 * LANES), dtype)
    return pl.pallas_call(
        functools.partial(column_layer, G, n, B),
        out_shape=jax.ShapeDtypeStruct((h * rows, columns), dtype),
        in_specs=[ANY] * 4,
        out_specs=pl.BlockSpec(memory_space=pltpu.VMEM),
        scratch_shapes=[
            pltpu.VMEM((2, half, 2 * depth), dtype),
            pltpu.VMEM((chunks, 2 * depth, 2 * LANES), dtype),
            pltpu.VMEM((chunks, B * LANES, columns), dtype),
            pltpu.VMEM((chunks, half, 2 * LANES), jnp.float32),
            pair, pair, pair, pair,
            pltpu.VMEM((chunks, half, LANES), dtype),
            pltpu.VMEM((2, chunks, half, B * LANES), dtype),
            pltpu.VMEM((2, half, columns), jnp.float32),
            DMA((chunks, 2)), DMA((2,)), DMA((chunks,)),
            DMA((chunks, 2)), DMA((chunks, 2)),
            DMA((G, chunks)), DMA((G, chunks)),
            DMA((4,)), DMA((4,)), DMA((4,)), DMA((4,)),
            DMA((chunks,)), DMA((chunks,)),
            DMA((chunks,)), DMA((chunks,)),
            DMA((chunks,)), DMA((chunks,)),
            DMA((chunks, 3)), DMA((chunks, B)),
            DMA((chunks,)), DMA((chunks,)),
            DMA((chunks,)), DMA((chunks,)),
        ],
        compiler_params=pltpu.CompilerParams(
            collective_id=0, has_side_effects=True, vmem_limit_bytes=63_000_000
        ),
        name="layer",
    )(tokens, gate_weight, up_weight, down_weight)


def solution(mesh):
    shape = dict(mesh.shape)
    sizes = shape["groups"], shape["tp"], shape["blk"]
    kernel = column_local if sizes[1:] == (8, 2) else local
    return jax.shard_map(
        functools.partial(kernel, *sizes),
        mesh=mesh,
        in_specs=(P(("groups", "tp"), None), P("tp", "blk"), P("tp", "blk"), P("blk", "tp")),
        out_specs=P(("groups", "blk"), "tp"),
        check_vma=False,
    )
```

```python
import functools

import jax
import jax.numpy as jnp
from jax import lax
from jax.experimental import pallas as pl
from jax.experimental.pallas import tpu as pltpu
from jax.sharding import PartitionSpec as P

MESH = pl.DeviceIdType.MESH
ANY = pl.BlockSpec(memory_space=pl.ANY)


def flip1(i):
    return i + 1 - 2 * (i % 2)


def greet(devices):
    barrier = pltpu.get_barrier_semaphore()
    for device in devices:
        pl.semaphore_signal(barrier, inc=1, device_id=device, device_id_type=MESH)
    pl.semaphore_wait(barrier, len(devices))


def flip2(i):
    return i + 2 - 4 * ((i // 2) % 2)


CUT = 8


def layer(
    G, n, B,
    tok, gate, up, down, out,
    T, W, D, both, mine_h, H, total,
    lsem, tok_send, tok_recv, core_send, core_recv,
    w_send, w_recv, x_send, x_recv, d_send, d_recv,
    h_send, h_recv, f_send, f_recv,
):
    g, t, b = lax.axis_index("groups"), lax.axis_index("tp"), lax.axis_index("blk")
    h = n // B
    a, j = t // h, t % h
    half, pairs = h // 2, n // 2
    p, y = t // 2, t % 2
    other = (g, t, 1 - b)
    across = (g, flip1(t), b)
    R, K = tok.shape
    width = K // B
    depth, units = gate.shape[0], gate.shape[1] // h
    part = depth // G
    mine = pl.ds(pl.multiple_of(b * width, 128), width)
    theirs = pl.ds(pl.multiple_of((1 - b) * width, 128), width)
    square = h == 4
    cut = R * CUT // 16
    upper, lower_rows = pl.ds(0, cut), pl.ds(cut, R - cut)

    greet(
        [(g, (t + d) % n, b) for d in range(1, n)]
        + [(g, 2 * ((p + d) % pairs) + y, 1 - b) for d in range(1, pairs)]
        + [((g + e) % G, t, b) for e in range(1, G)]
        + [other]
    )

    def remote(src, dst, send, recv, device):
        return pltpu.make_async_remote_copy(
            src_ref=src, dst_ref=dst, send_sem=send, recv_sem=recv,
            device_id=device, device_id_type=MESH,
        )

    pending = []

    def push(*copy):
        c = remote(*copy)
        c.start()
        pending.append(c)

    def local(src, dst, sem):
        return pltpu.make_async_copy(src, dst, sem)

    def rows_of(i, s):
        if square:
            i = flip1(i) if s % 2 else i
            return flip2(i) if s // 2 else i
        return (i + h - s) % h

    def token_block(s):
        return T.at[rows_of(j, s), :, mine]

    def w_block(source, first, size, k):
        start = pl.multiple_of(source * depth + first, 16)
        return W.at[pl.ds(start, size), pl.ds(k * units, units)]

    own_columns = pl.ds(pl.multiple_of(j * units, 128), units)
    loads = [
        local(gate.at[:, own_columns], w_block(t, 0, depth, 0), lsem.at[0]),
        local(up.at[:, own_columns], w_block(t, 0, depth, 1), lsem.at[1]),
        local(tok, T.at[j], lsem.at[2]),
        local(down, D.at[b], lsem.at[3]),
    ]

    first = g * part
    rows = pl.ds(pl.multiple_of(first, 16), part)
    order = [d for k in range(1, n // 2) for d in (k, n - k)] + [n // 2]
    for d in order:
        dest = (t + d) % n
        cols = pl.ds(pl.multiple_of((dest % h) * units, 128), units)
        for k in range(2):
            push(
                (gate, up)[k].at[rows, cols], w_block(t, first, part, k),
                w_send.at[d, k], w_recv.at[d, k], (g, dest, b),
            )

    for s in (2, 1) if square else range(1, h):
        dest = rows_of(j, s) if square else (j + s) % h
        push(tok.at[:, mine], T.at[j, :, mine], tok_send.at[s], tok_recv.at[s], (g, a * h + dest, b))
    push(down, D.at[b], d_send, d_recv, other)
    for load in loads:
        load.start()

    for d in order:
        source = (t + n - d) % n
        for k in range(2):
            block = w_block(source, first, part, k)
            remote(block, block, w_send.at[d, k], w_recv.at[d, k], other).wait_recv()
            for e in range(1, G):
                push(block, block, x_send.at[e, d, k], x_recv.at[e, d, k], ((g + e) % G, t, b))
    for load in loads:
        load.wait()
    remote(D.at[1 - b], D.at[1 - b], d_send, d_recv, other).wait_recv()
    total[...] = jnp.zeros_like(total)

    def tokens_arrive(s):
        block = token_block(s)
        if square and s == 3:
            for i, r in ((3, upper), (0, lower_rows)):
                piece = T.at[rows_of(j, s), r, mine]
                remote(piece, piece, tok_send.at[i], tok_recv.at[i], other).wait_recv()
        else:
            remote(block, block, tok_send.at[s], tok_recv.at[s], other).wait_recv()
        if square and s < 3:
            piece = T.at[rows_of(j, s), (upper, lower_rows)[s - 1], mine]
            target = flip2(j) if s == 1 else flip1(j)
            i = 3 if s == 1 else 0
            push(piece, piece, tok_send.at[i], tok_recv.at[i], (g, a * h + target, b))

        push(block, block, core_send.at[s], core_recv.at[s], other)

    def compute(s):
        slot = rows_of(j, s)
        if s > 0:
            block = T.at[slot, :, theirs]
            remote(block, block, core_send.at[s], core_recv.at[s], other).wait_recv()
        tiles = 4 if K % 512 == 0 else 1
        tile = K // tiles
        both[...] = jnp.zeros_like(both)

        def body(i, carry):
            k = pl.ds(pl.multiple_of(i * tile, 128), tile)
            both[...] += jnp.dot(T[slot, :, k], W[k, :], preferred_element_type=jnp.float32)
            return carry

        lax.fori_loop(0, tiles, body, 0)
        hidden = (jax.nn.silu(both[:, :units]) * both[:, units:]).astype(out.dtype)
        mine_h[s] = hidden

        @pl.when(a == b)
        def _():
            H[s, j, b] = hidden

        for d in sorted(range(1, pairs), key=lambda d: min(d, pairs - d)):
            push(
                mine_h.at[s], H.at[s, j, b], h_send.at[s, d], h_recv.at[s, j // 2, b],
                (g, 2 * ((p + d) % pairs) + y, a),
            )

        @pl.when(a != b)
        def _():
            remote(mine_h.at[s], H.at[s, j, b], h_send.at[s, 0], h_recv.at[s, j // 2, b], other).start()

    def pass_on(s):
        for k in range(half):
            for c in range(B):
                block = H.at[s, 2 * k + y, c]

                @pl.when(jnp.logical_not((a == b) & (j // 2 == k) & (c == b)))
                def _():
                    remote(block, block, h_send.at[s, 0], h_recv.at[s, k, c], other).wait_recv()

                push(block, block, f_send.at[s, k, c], f_recv.at[s, k, c], across)

    def lower(s):
        for k in range(half):
            for c in range(B):
                block = H.at[s, 2 * k + 1 - y, c]
                remote(block, block, f_send.at[s, k, c], f_recv.at[s, k, c], across).wait_recv()

        def body(i, carry):
            r = rows_of(i, s)
            term = total[r]
            for c in range(B):
                term += jnp.dot(
                    H[s, i, c], D[c, pl.ds(pl.multiple_of(i * units, 128), units), :],
                    preferred_element_type=jnp.float32,
                )
            total[r] = term
            return carry

        lax.fori_loop(0, h, body, 0)

    for d in order:
        source = (t + n - d) % n
        for e in range(1, G):
            for k in range(2):
                block = w_block(source, ((g + G - e) % G) * part, part, k)
                remote(block, block, x_send.at[e, d, k], x_recv.at[e, d, k], other).wait_recv()

    compute(0)
    for s in range(1, h):
        tokens_arrive(s)
        compute(s)
        pass_on(s - 1)
        if s >= 2:
            lower(s - 2)
    pass_on(h - 1)
    lower(h - 2)
    lower(h - 1)
    for r in range(h):
        out[pl.ds(r * R, R), :] = total[r].astype(out.dtype)

    for c in pending:
        c.wait_send()
    @pl.when(a != b)
    def _():
        for s in range(h):
            remote(mine_h.at[s], mine_h.at[s], h_send.at[s, 0], h_recv.at[s, 0, 0], other).wait_send()


def local(G, n, B, tokens, gate_weight, up_weight, down_weight):
    h = n // B
    R, K = tokens.shape
    depth, wide = gate_weight.shape
    units, columns = wide // h, down_weight.shape[1]
    dtype = tokens.dtype
    DMA = pltpu.SemaphoreType.DMA
    return pl.pallas_call(
        functools.partial(layer, G, n, B),
        out_shape=jax.ShapeDtypeStruct((h * R, columns), dtype),
        in_specs=[ANY] * 4,
        out_specs=pl.BlockSpec(memory_space=pltpu.VMEM),
        scratch_shapes=[
            pltpu.VMEM((h, R, K), dtype),
            pltpu.VMEM((K, 2 * units), dtype),
            pltpu.VMEM((B, wide, columns), dtype),
            pltpu.VMEM((R, 2 * units), jnp.float32),
            pltpu.VMEM((h, R, units), dtype),
            pltpu.VMEM((h, h, B, R, units), dtype),
            pltpu.VMEM((h, R, columns), jnp.float32),
            DMA((4,)),
            DMA((h,)), DMA((h,)), DMA((h,)), DMA((h,)),
            DMA((n, 2)), DMA((n, 2)),
            DMA((G, n, 2)), DMA((G, n, 2)),
            DMA, DMA,
            DMA((h, n // 2)), DMA((h, h // 2, B)),
            DMA((h, h // 2, B)), DMA((h, h // 2, B)),
        ],
        compiler_params=pltpu.CompilerParams(
            collective_id=0, has_side_effects=True, vmem_limit_bytes=63_000_000
        ),
        name="layer",
    )(tokens, gate_weight, up_weight, down_weight)


LANES = 128


def column_layer(
    G, n, B,
    tok, gate, up, down, out,
    X, W, D, Q, S, R, hs, H, acc,
    l_w, l_x, l_d,
    p_send, p_recv, q_send, q_recv, f_send, f_recv, x_send, x_recv,
    t_send, t_recv, c_send, c_recv, d_send, d_recv,
    z_send, z_recv, h_send, h_recv, r_send, r_recv, y_send, y_recv,
):
    g, t, b = lax.axis_index("groups"), lax.axis_index("tp"), lax.axis_index("blk")
    h = n // B
    z, y, j, a = t // 2, t % 2, t % h, t // h
    last = n // 2 - 1
    mz = last - z
    inner = z % 2 + a == 1
    outer = z % 2 + a != 1
    own, foreign = b == a, b != a
    rows, depth, wide = tok.shape[0], gate.shape[0], gate.shape[1]
    part, run, half = depth // G, 2 * depth, h // 2 * rows
    chunks = wide // LANES // 2
    other = (g, t, 1 - b)
    beside = (g, flip1(t), b)
    along = flip2(t)
    facing = 2 * mz + y

    greet(
        [(g, chip, c) for chip in (along, facing) for c in range(B)]
        + [other, beside]
        + [((g + e) % G, t, b) for e in range(1, G)]
    )

    def remote(src, dst, send, recv, device):
        return pltpu.make_async_remote_copy(
            src_ref=src, dst_ref=dst, send_sem=send, recv_sem=recv,
            device_id=device, device_id_type=MESH,
        )

    def push(*copy):
        remote(*copy).start()

    def got(ref, sem):
        remote(ref, ref, sem, sem, other).wait_recv()

    def sent(ref, sem):
        remote(ref, ref, sem, sem, other).wait_send()

    def lanes(k):
        return pl.ds(pl.multiple_of(k * LANES, LANES), LANES)

    share = pl.ds(pl.multiple_of(g * part, 16), part)

    def landing(k, e):
        return pl.ds(pl.multiple_of(k * depth + e * part, 16), part)

    def w_piece(c, slot, k):
        return W.at[c, landing(slot, g), pl.ds(k * LANES, LANES)]

    def w_share(c, slot, e):
        return W.at[c, landing(slot, e), :]

    def depth_of(row):
        return pl.ds(pl.multiple_of(row * run, LANES), run)

    def x_block(i, k):
        return X.at[
            i // 2, pl.ds(pl.multiple_of(i % 2 * rows, 16), rows),
            pl.ds(pl.multiple_of(k * run, LANES), run),
        ]

    def d_block(i, k):
        return D.at[i, pl.ds(pl.multiple_of(k * LANES, LANES), LANES), :]

    near, beyond, diagonal = flip1(j), flip2(j), flip1(flip2(j))
    z2 = along // 2
    row_there = z2 + b * (last - 2 * z2)
    row_here = z + b * (mz - z)

    def send_across(c):
        for k in range(2):
            push(
                (gate, up)[k].at[share, lanes(y * chunks + c)], w_piece(c, 2 + y, k),
                p_send.at[c, k], p_recv.at[c, k], (g, facing, b),
            )

    def send_beside(c):
        for k in range(2):
            push(
                (gate, up)[k].at[share, lanes((1 - y) * chunks + c)], w_piece(c, y, k),
                q_send.at[c, k], q_recv.at[c, k], beside,
            )

    push(tok.at[:, depth_of(row_there)], x_block(j, b), t_send.at[0], t_recv.at[0], (g, along, b))
    send_beside(0)
    push(tok.at[:, depth_of(row_here)], x_block(j, b), t_send.at[1], t_recv.at[1], beside)
    send_beside(1)

    @pl.when(inner)
    def _():
        send_across(0)
        send_across(1)

    loads = []
    for k, row in enumerate((z, mz)):
        loads.append(pltpu.make_async_copy(tok.at[:, depth_of(row)], x_block(j, k), l_x.at[k]))
    for c in range(chunks):
        for k in range(2):
            loads.append(pltpu.make_async_copy(
                (gate, up)[k].at[:, lanes(y * chunks + c)],
                W.at[c, pl.ds(pl.multiple_of(y * depth, LANES), depth), pl.ds(k * LANES, LANES)],
                l_w.at[c, k],
            ))
    for i in range(2 * chunks):
        piece = down.at[pl.ds(i * LANES, LANES), :]
        loads.append(pltpu.make_async_copy(piece, d_block(i, b), l_d.at[i]))
        push(piece, d_block(i, b), d_send.at[i], d_recv.at[i], other)
    for load in loads:
        load.start()
    acc[...] = jnp.zeros_like(acc)

    def swap(c, slot, i):
        block = w_share(c, slot, g)
        for e in range(1, G):
            push(block, block, x_send.at[e, c, i], x_recv.at[e, c, i], ((g + e) % G, t, b))

    def from_beside(c):
        for k in range(2):
            got(w_piece(c, 1 - y, k), q_recv.at[c, k])
        swap(c, 1 - y, 0)

    def relay(c):
        push(w_share(c, 1 - y, g), w_share(c, 3 - y, g), f_send.at[c], f_recv.at[c], (g, facing, b))

    def from_facing(c):
        for k in range(2):
            got(w_piece(c, 2 + y, k), p_recv.at[c, k])
        swap(c, 2 + y, 1)

    def relayed(c):
        got(w_share(c, 3 - y, g), f_recv.at[c])
        swap(c, 3 - y, 2)

    def pass_tokens(i, k):
        block = x_block(i, b)
        got(block, t_recv.at[k])
        push(block, block, c_send.at[k], c_recv.at[k], other)

    def ready(c):
        for e in range(1, G):
            for i, slot in enumerate((1 - y, 2 + y, 3 - y)):
                got(w_share(c, slot, (g + G - e) % G), x_recv.at[e, c, i])

    def multiply(c, r):
        return jnp.dot(X[r], W[c], preferred_element_type=jnp.float32)

    def keep(c, r):
        Q[c, r] = multiply(c, r)

    def give(c, r):
        S[c, r] = multiply(c, r).astype(S.dtype)
        push(S.at[c, r], R.at[c, r], z_send.at[c, r], z_recv.at[c, r], (g, along, b))

    def h_piece(c, r, k):
        return H.at[y, c, r, :, lanes(k)]

    def finish(c, r):
        got(R.at[c, r], z_recv.at[c, r])
        both = Q[c, r] + R[c, r].astype(jnp.float32)
        hidden = (jax.nn.silu(both[:, :LANES]) * both[:, LANES:]).astype(hs.dtype)
        hs[c, r] = hidden
        block, there = hs.at[c, r], h_piece(c, r, b)
        push(block, there, h_send.at[c, r, 0], h_recv.at[c, r, b], (g, facing, a))
        push(block, there, h_send.at[c, r, 1], h_recv.at[c, r, b], (g, along, a))

        @pl.when(own)
        def _():
            H[y, c, r, :, lanes(b)] = hidden

        @pl.when(foreign)
        def _():
            push(block, there, h_send.at[c, r, 2], h_recv.at[c, r, b], other)

    def onward(c, r):
        push(H.at[y, c, r], H.at[y, c, r], y_send.at[c, r], y_recv.at[c, r], beside)

    def spread_own_inner(c, r):
        got(h_piece(c, r, 1 - b), h_recv.at[c, r, 1 - b])
        onward(c, r)

    def spread_own_outer(c, r):
        for k in range(B):
            got(h_piece(c, r, k), h_recv.at[c, r, k])
        onward(c, r)

    def spread_foreign_inner(c, r):
        for k in range(B):
            got(h_piece(c, r, k), h_recv.at[c, r, k])
        block = H.at[y, c, r]
        push(block, block, r_send.at[c, r], r_recv.at[c, r], (g, along, b))
        onward(c, r)

    def spread_foreign_outer(c, r):
        got(H.at[y, c, r], r_recv.at[c, r])
        onward(c, r)

    def project(c, r):
        got(H.at[1 - y, c, r], y_recv.at[c, r])
        acc[r] += jnp.dot(H[0, c, r], D[c], preferred_element_type=jnp.float32) + jnp.dot(
            H[1, c, r], D[chunks + c], preferred_element_type=jnp.float32
        )

    rz = z % 2

    def pass_beyond():
        block = x_block(beyond, b)
        got(block, t_recv.at[0])
        push(block, block, t_send.at[2], t_recv.at[2], beside)
        push(block, block, c_send.at[0], c_recv.at[0], other)
        for c in range(2, chunks):
            send_beside(c)

    def held(i, k):
        got(x_block(i, 1 - b), c_recv.at[k])

    def settle():
        for load in loads:
            load.wait()

    def settle_down():
        for i in range(2 * chunks):
            got(d_block(i, 1 - b), d_recv.at[i])

    def when(role, stage, *args):
        @pl.when(role)
        def _():
            stage(*args)

    halves = (rz, 1 - rz)
    end = chunks - 1

    def tokens_complete():
        pass_tokens(diagonal, 2)
        held(beyond, 0)
        held(diagonal, 2)

    def each(stage, c, order):
        for r in order:
            stage(c, r)

    @pl.when(inner)
    def _():
        first = (1 - rz, rz)
        from_beside(0)
        relay(0)
        send_across(2)
        from_facing(0)
        from_facing(1)
        relayed(0)
        pass_beyond()
        pass_tokens(near, 1)
        settle()
        held(near, 1)
        ready(0)
        keep(0, rz)
        from_beside(1)
        relay(1)
        tokens_complete()
        keep(0, 1 - rz)
        finish(0, 1 - rz)
        from_beside(2)
        relay(2)
        send_across(3)
        when(own, spread_own_inner, 0, 1 - rz)
        finish(0, rz)
        from_beside(3)
        relay(3)
        when(own, spread_own_inner, 0, rz)
        settle_down()
        relayed(1)
        from_facing(2)
        when(own, project, 0, 1 - rz)
        ready(1)
        each(keep, 1, first)
        relayed(2)
        each(finish, 1, first)
        when(own, each, spread_own_inner, 1, first)
        from_facing(3)
        when(foreign, each, spread_foreign_inner, 0, halves)
        ready(2)
        each(keep, 2, first)
        relayed(3)
        each(finish, 2, first)
        when(own, each, spread_own_inner, 2, first)
        when(own, project, 0, rz)
        when(foreign, each, spread_foreign_inner, 1, halves)
        ready(3)
        each(keep, 3, first)

        @pl.when(own)
        def _():
            each(project, 1, first)
            for r in first:
                finish(3, r)
                spread_own_inner(3, r)
            for c in (2, 3):
                each(project, c, first)

        @pl.when(foreign)
        def _():
            each(project, 0, halves)
            spread_foreign_inner(2, rz)
            finish(3, 1 - rz)
            spread_foreign_inner(2, 1 - rz)
            finish(3, rz)
            each(project, 1, halves)
            each(spread_foreign_inner, 3, halves)
            each(project, 2, halves)
            each(project, 3, halves)

    @pl.when(outer)
    def _():
        far = (1 - rz, rz)
        from_beside(0)
        sent(x_block(j, 0), t_send.at[0])
        send_across(0)
        relay(0)
        send_across(1)
        pass_beyond()
        pass_tokens(near, 1)
        from_facing(0)
        from_beside(1)
        relay(1)
        for c in range(2, chunks):
            send_across(c)
        relayed(0)
        from_facing(1)
        settle()
        held(near, 1)
        ready(0)
        give(0, rz)
        relayed(1)
        tokens_complete()
        give(0, 1 - rz)
        from_facing(2)
        from_beside(2)
        relay(2)
        ready(1)
        give(1, rz)
        from_beside(3)
        relay(3)
        give(1, 1 - rz)
        from_facing(3)
        settle_down()
        relayed(2)
        when(own, spread_own_outer, 0, rz)
        relayed(3)
        ready(2)
        each(give, 2, halves)
        ready(3)
        each(give, 3, halves)
        when(own, spread_own_outer, 0, 1 - rz)

        @pl.when(own)
        def _():
            for c in (1, 2, 3):
                each(spread_own_outer, c, halves)
                each(project, c - 1, halves)
            each(project, 3, halves)

        @pl.when(foreign)
        def _():
            each(spread_foreign_outer, 0, far)
            for c in (1, 2, 3):
                each(spread_foreign_outer, c, far)
                each(project, c - 1, far)
            each(project, 3, far)

    for r in range(2):
        out[pl.ds(r * half, half), :] = acc[r].astype(out.dtype)

    when(inner, sent, x_block(j, 0), t_send.at[0])
    for k in range(3):
        if k:
            sent(x_block(j, 0), t_send.at[k])
        sent(x_block(j, 0), c_send.at[k])
    for i in range(2 * chunks):
        sent(d_block(i, b), d_send.at[i])

    def drain(c, carry):
        for k in range(2):
            sent(w_piece(c, 0, k), p_send.at[c, k])
            sent(w_piece(c, 0, k), q_send.at[c, k])
        sent(w_share(c, 0, g), f_send.at[c])
        for e in range(1, G):
            for i in range(3):
                sent(w_share(c, 0, g), x_send.at[e, c, i])
        for r in range(2):
            sent(H.at[y, c, r], y_send.at[c, r])

            @pl.when(outer)
            def _():
                sent(S.at[c, r], z_send.at[c, r])

            @pl.when(inner)
            def _():
                sent(hs.at[c, r], h_send.at[c, r, 0])
                sent(hs.at[c, r], h_send.at[c, r, 1])

            @pl.when(jnp.logical_and(inner, foreign))
            def _():
                sent(hs.at[c, r], h_send.at[c, r, 2])
                sent(H.at[y, c, r], r_send.at[c, r])

        return carry

    lax.fori_loop(0, chunks, drain, 0)


def column_local(G, n, B, tokens, gate_weight, up_weight, down_weight):
    h = n // B
    rows = tokens.shape[0]
    depth, wide = gate_weight.shape
    columns = down_weight.shape[1]
    chunks = wide // LANES // 2
    half = h // 2 * rows
    dtype = tokens.dtype
    DMA = pltpu.SemaphoreType.DMA
    pair = pltpu.VMEM((chunks, 2, half, 2 * LANES), dtype)
    return pl.pallas_call(
        functools.partial(column_layer, G, n, B),
        out_shape=jax.ShapeDtypeStruct((h * rows, columns), dtype),
        in_specs=[ANY] * 4,
        out_specs=pl.BlockSpec(memory_space=pltpu.VMEM),
        scratch_shapes=[
            pltpu.VMEM((2, half, 4 * depth), dtype),
            pltpu.VMEM((chunks, 4 * depth, 2 * LANES), dtype),
            pltpu.VMEM((2 * chunks, B * LANES, columns), dtype),
            pltpu.VMEM((chunks, 2, half, 2 * LANES), jnp.float32),
            pair, pair,
            pltpu.VMEM((chunks, 2, half, LANES), dtype),
            pltpu.VMEM((2, chunks, 2, half, B * LANES), dtype),
            pltpu.VMEM((2, half, columns), jnp.float32),
            DMA((chunks, 2)), DMA((2,)), DMA((2 * chunks,)),
            DMA((chunks, 2)), DMA((chunks, 2)),
            DMA((chunks, 2)), DMA((chunks, 2)),
            DMA((chunks,)), DMA((chunks,)),
            DMA((G, chunks, 3)), DMA((G, chunks, 3)),
            DMA((3,)), DMA((3,)), DMA((3,)), DMA((3,)),
            DMA((2 * chunks,)), DMA((2 * chunks,)),
            DMA((chunks, 2)), DMA((chunks, 2)),
            DMA((chunks, 2, 3)), DMA((chunks, 2, B)),
            DMA((chunks, 2)), DMA((chunks, 2)),
            DMA((chunks, 2)), DMA((chunks, 2)),
        ],
        compiler_params=pltpu.CompilerParams(
            collective_id=0, has_side_effects=True, vmem_limit_bytes=63_000_000
        ),
        name="layer",
    )(tokens, gate_weight, up_weight, down_weight)


def solution(mesh):
    shape = dict(mesh.shape)
    sizes = shape["groups"], shape["tp"], shape["blk"]
    kernel = column_local if sizes[1:] == (8, 2) else local
    return jax.shard_map(
        functools.partial(kernel, *sizes),
        mesh=mesh,
        in_specs=(P(("groups", "tp"), None), P("tp", "blk"), P("tp", "blk"), P("blk", "tp")),
        out_specs=P(("groups", "blk"), "tp"),
        check_vma=False,
    )
```

```python
import functools

import jax
import jax.numpy as jnp
from jax import lax
from jax.experimental import pallas as pl
from jax.experimental.pallas import tpu as pltpu
from jax.sharding import PartitionSpec as P

MESH = pl.DeviceIdType.MESH
ANY = pl.BlockSpec(memory_space=pl.ANY)


def flip1(i):
    return i + 1 - 2 * (i % 2)


def greet(devices):
    barrier = pltpu.get_barrier_semaphore()
    for device in devices:
        pl.semaphore_signal(barrier, inc=1, device_id=device, device_id_type=MESH)
    pl.semaphore_wait(barrier, len(devices))


def flip2(i):
    return i + 2 - 4 * ((i // 2) % 2)


CUT = 8


def layer(
    G, n, B,
    tok, gate, up, down, out,
    T, W, D, both, mine_h, H, total,
    lsem, tok_send, tok_recv, core_send, core_recv,
    w_send, w_recv, x_send, x_recv, d_send, d_recv,
    h_send, h_recv, f_send, f_recv,
):
    g, t, b = lax.axis_index("groups"), lax.axis_index("tp"), lax.axis_index("blk")
    h = n // B
    a, j = t // h, t % h
    half, pairs = h // 2, n // 2
    p, y = t // 2, t % 2
    other = (g, t, 1 - b)
    across = (g, flip1(t), b)
    R, K = tok.shape
    width = K // B
    depth, units = gate.shape[0], gate.shape[1] // h
    part = depth // G
    mine = pl.ds(pl.multiple_of(b * width, 128), width)
    theirs = pl.ds(pl.multiple_of((1 - b) * width, 128), width)
    square = h == 4
    cut = R * CUT // 16
    upper, lower_rows = pl.ds(0, cut), pl.ds(cut, R - cut)

    greet(
        [(g, (t + d) % n, b) for d in range(1, n)]
        + [(g, 2 * ((p + d) % pairs) + y, 1 - b) for d in range(1, pairs)]
        + [((g + e) % G, t, b) for e in range(1, G)]
        + [other]
    )

    def remote(src, dst, send, recv, device):
        return pltpu.make_async_remote_copy(
            src_ref=src, dst_ref=dst, send_sem=send, recv_sem=recv,
            device_id=device, device_id_type=MESH,
        )

    pending = []

    def push(*copy):
        c = remote(*copy)
        c.start()
        pending.append(c)

    def local(src, dst, sem):
        return pltpu.make_async_copy(src, dst, sem)

    def rows_of(i, s):
        if square:
            i = flip1(i) if s % 2 else i
            return flip2(i) if s // 2 else i
        return (i + h - s) % h

    def token_block(s):
        return T.at[rows_of(j, s), :, mine]

    def w_block(source, first, size, k):
        start = pl.multiple_of(source * depth + first, 16)
        return W.at[pl.ds(start, size), pl.ds(k * units, units)]

    own_columns = pl.ds(pl.multiple_of(j * units, 128), units)
    loads = [
        local(gate.at[:, own_columns], w_block(t, 0, depth, 0), lsem.at[0]),
        local(up.at[:, own_columns], w_block(t, 0, depth, 1), lsem.at[1]),
        local(tok, T.at[j], lsem.at[2]),
        local(down, D.at[b], lsem.at[3]),
    ]

    first = g * part
    rows = pl.ds(pl.multiple_of(first, 16), part)
    order = [d for k in range(1, n // 2) for d in (k, n - k)] + [n // 2]
    for d in order:
        dest = (t + d) % n
        cols = pl.ds(pl.multiple_of((dest % h) * units, 128), units)
        for k in range(2):
            push(
                (gate, up)[k].at[rows, cols], w_block(t, first, part, k),
                w_send.at[d, k], w_recv.at[d, k], (g, dest, b),
            )

    for s in (2, 1) if square else range(1, h):
        dest = rows_of(j, s) if square else (j + s) % h
        push(tok.at[:, mine], T.at[j, :, mine], tok_send.at[s], tok_recv.at[s], (g, a * h + dest, b))
    push(down, D.at[b], d_send, d_recv, other)
    for load in loads:
        load.start()

    for d in order:
        source = (t + n - d) % n
        for k in range(2):
            block = w_block(source, first, part, k)
            remote(block, block, w_send.at[d, k], w_recv.at[d, k], other).wait_recv()
            for e in range(1, G):
                push(block, block, x_send.at[e, d, k], x_recv.at[e, d, k], ((g + e) % G, t, b))
    for load in loads:
        load.wait()
    remote(D.at[1 - b], D.at[1 - b], d_send, d_recv, other).wait_recv()
    total[...] = jnp.zeros_like(total)

    def tokens_arrive(s):
        block = token_block(s)
        if square and s == 3:
            for i, r in ((3, upper), (0, lower_rows)):
                piece = T.at[rows_of(j, s), r, mine]
                remote(piece, piece, tok_send.at[i], tok_recv.at[i], other).wait_recv()
        else:
            remote(block, block, tok_send.at[s], tok_recv.at[s], other).wait_recv()
        if square and s < 3:
            piece = T.at[rows_of(j, s), (upper, lower_rows)[s - 1], mine]
            target = flip2(j) if s == 1 else flip1(j)
            i = 3 if s == 1 else 0
            push(piece, piece, tok_send.at[i], tok_recv.at[i], (g, a * h + target, b))

        push(block, block, core_send.at[s], core_recv.at[s], other)

    def compute(s):
        slot = rows_of(j, s)
        if s > 0:
            block = T.at[slot, :, theirs]
            remote(block, block, core_send.at[s], core_recv.at[s], other).wait_recv()
        tiles = 4 if K % 512 == 0 else 1
        tile = K // tiles
        both[...] = jnp.zeros_like(both)

        def body(i, carry):
            k = pl.ds(pl.multiple_of(i * tile, 128), tile)
            both[...] += jnp.dot(T[slot, :, k], W[k, :], preferred_element_type=jnp.float32)
            return carry

        lax.fori_loop(0, tiles, body, 0)
        hidden = (jax.nn.silu(both[:, :units]) * both[:, units:]).astype(out.dtype)
        mine_h[s] = hidden

        @pl.when(a == b)
        def _():
            H[s, j, b] = hidden

        for d in sorted(range(1, pairs), key=lambda d: min(d, pairs - d)):
            push(
                mine_h.at[s], H.at[s, j, b], h_send.at[s, d], h_recv.at[s, j // 2, b],
                (g, 2 * ((p + d) % pairs) + y, a),
            )

        @pl.when(a != b)
        def _():
            remote(mine_h.at[s], H.at[s, j, b], h_send.at[s, 0], h_recv.at[s, j // 2, b], other).start()

    def pass_on(s):
        for k in range(half):
            for c in range(B):
                block = H.at[s, 2 * k + y, c]

                @pl.when(jnp.logical_not((a == b) & (j // 2 == k) & (c == b)))
                def _():
                    remote(block, block, h_send.at[s, 0], h_recv.at[s, k, c], other).wait_recv()

                push(block, block, f_send.at[s, k, c], f_recv.at[s, k, c], across)

    def lower(s):
        for k in range(half):
            for c in range(B):
                block = H.at[s, 2 * k + 1 - y, c]
                remote(block, block, f_send.at[s, k, c], f_recv.at[s, k, c], across).wait_recv()

        def body(i, carry):
            r = rows_of(i, s)
            term = total[r]
            for c in range(B):
                term += jnp.dot(
                    H[s, i, c], D[c, pl.ds(pl.multiple_of(i * units, 128), units), :],
                    preferred_element_type=jnp.float32,
                )
            total[r] = term
            return carry

        lax.fori_loop(0, h, body, 0)

    for d in order:
        source = (t + n - d) % n
        for e in range(1, G):
            for k in range(2):
                block = w_block(source, ((g + G - e) % G) * part, part, k)
                remote(block, block, x_send.at[e, d, k], x_recv.at[e, d, k], other).wait_recv()

    compute(0)
    for s in range(1, h):
        tokens_arrive(s)
        compute(s)
        pass_on(s - 1)
        if s >= 2:
            lower(s - 2)
    pass_on(h - 1)
    lower(h - 2)
    lower(h - 1)
    for r in range(h):
        out[pl.ds(r * R, R), :] = total[r].astype(out.dtype)

    for c in pending:
        c.wait_send()
    @pl.when(a != b)
    def _():
        for s in range(h):
            remote(mine_h.at[s], mine_h.at[s], h_send.at[s, 0], h_recv.at[s, 0, 0], other).wait_send()


def local(G, n, B, tokens, gate_weight, up_weight, down_weight):
    h = n // B
    R, K = tokens.shape
    depth, wide = gate_weight.shape
    units, columns = wide // h, down_weight.shape[1]
    dtype = tokens.dtype
    DMA = pltpu.SemaphoreType.DMA
    return pl.pallas_call(
        functools.partial(layer, G, n, B),
        out_shape=jax.ShapeDtypeStruct((h * R, columns), dtype),
        in_specs=[ANY] * 4,
        out_specs=pl.BlockSpec(memory_space=pltpu.VMEM),
        scratch_shapes=[
            pltpu.VMEM((h, R, K), dtype),
            pltpu.VMEM((K, 2 * units), dtype),
            pltpu.VMEM((B, wide, columns), dtype),
            pltpu.VMEM((R, 2 * units), jnp.float32),
            pltpu.VMEM((h, R, units), dtype),
            pltpu.VMEM((h, h, B, R, units), dtype),
            pltpu.VMEM((h, R, columns), jnp.float32),
            DMA((4,)),
            DMA((h,)), DMA((h,)), DMA((h,)), DMA((h,)),
            DMA((n, 2)), DMA((n, 2)),
            DMA((G, n, 2)), DMA((G, n, 2)),
            DMA, DMA,
            DMA((h, n // 2)), DMA((h, h // 2, B)),
            DMA((h, h // 2, B)), DMA((h, h // 2, B)),
        ],
        compiler_params=pltpu.CompilerParams(
            collective_id=0, has_side_effects=True, vmem_limit_bytes=63_000_000
        ),
        name="layer",
    )(tokens, gate_weight, up_weight, down_weight)


LANES = 128


def column_layer(
    G, n, B,
    tok, gate, up, down, out,
    X, W, D, Q, S, R, hs, H, acc,
    l_w, l_x, l_d,
    p_send, p_recv, q_send, q_recv, f_send, f_recv, x_send, x_recv,
    t_send, t_recv, c_send, c_recv, d_send, d_recv,
    z_send, z_recv, h_send, h_recv, r_send, r_recv, y_send, y_recv, word,
):
    g, t, b = lax.axis_index("groups"), lax.axis_index("tp"), lax.axis_index("blk")
    h = n // B
    z, y, j, a = t // 2, t % 2, t % h, t // h
    last = n // 2 - 1
    mz = last - z
    inner = z % 2 + a == 1
    outer = z % 2 + a != 1
    own, foreign = b == a, b != a
    rows, depth, wide = tok.shape[0], gate.shape[0], gate.shape[1]
    part, run, half = depth // G, 2 * depth, h // 2 * rows
    chunks = wide // LANES // 2
    other = (g, t, 1 - b)
    beside = (g, flip1(t), b)
    along = flip2(t)
    facing = 2 * mz + y

    near_by = [(g, along, c) for c in range(B)] + [other, beside]
    near_by += [((g + e) % G, t, b) for e in range(1, G)]
    opposite = [(g, facing, c) for c in range(B)]

    @pl.when(inner)
    def _():
        greet(near_by + opposite)

    @pl.when(outer)
    def _():
        greet(near_by)

    def tell(device):
        pl.semaphore_signal(word, inc=1, device_id=device, device_id_type=MESH)

    def hear():
        pl.semaphore_wait(word, 1)

    def remote(src, dst, send, recv, device):
        return pltpu.make_async_remote_copy(
            src_ref=src, dst_ref=dst, send_sem=send, recv_sem=recv,
            device_id=device, device_id_type=MESH,
        )

    def push(*copy):
        remote(*copy).start()

    def got(ref, sem):
        remote(ref, ref, sem, sem, other).wait_recv()

    def sent(ref, sem):
        remote(ref, ref, sem, sem, other).wait_send()

    def lanes(k):
        return pl.ds(pl.multiple_of(k * LANES, LANES), LANES)

    share = pl.ds(pl.multiple_of(g * part, 16), part)

    def landing(k, e):
        return pl.ds(pl.multiple_of(k * depth + e * part, 16), part)

    def w_piece(c, slot, k):
        return W.at[c, landing(slot, g), pl.ds(k * LANES, LANES)]

    def w_share(c, slot, e):
        return W.at[c, landing(slot, e), :]

    def depth_of(row):
        return pl.ds(pl.multiple_of(row * run, LANES), run)

    def x_block(i, k):
        return X.at[
            i // 2, pl.ds(pl.multiple_of(i % 2 * rows, 16), rows),
            pl.ds(pl.multiple_of(k * run, LANES), run),
        ]

    def d_block(i, k):
        return D.at[i, pl.ds(pl.multiple_of(k * LANES, LANES), LANES), :]

    near, beyond, diagonal = flip1(j), flip2(j), flip1(flip2(j))
    z2 = along // 2
    row_there = z2 + b * (last - 2 * z2)
    row_here = z + b * (mz - z)

    def send_across(c):
        for k in range(2):
            push(
                (gate, up)[k].at[share, lanes(y * chunks + c)], w_piece(c, 2 + y, k),
                p_send.at[c, k], p_recv.at[c, k], (g, facing, b),
            )

    def send_beside(c):
        for k in range(2):
            push(
                (gate, up)[k].at[share, lanes((1 - y) * chunks + c)], w_piece(c, y, k),
                q_send.at[c, k], q_recv.at[c, k], beside,
            )

    push(tok.at[:, depth_of(row_there)], x_block(j, b), t_send.at[0], t_recv.at[0], (g, along, b))
    send_beside(0)
    send_beside(1)
    push(tok.at[:, depth_of(row_here)], x_block(j, b), t_send.at[1], t_recv.at[1], beside)
    send_beside(2)

    @pl.when(inner)
    def _():
        send_across(0)
        send_across(1)
        tell((g, facing, b))
        hear()
        tell((g, along, b))

    loads = []
    for k, row in enumerate((z, mz)):
        loads.append(pltpu.make_async_copy(tok.at[:, depth_of(row)], x_block(j, k), l_x.at[k]))
    for c in range(chunks):
        for k in range(2):
            loads.append(pltpu.make_async_copy(
                (gate, up)[k].at[:, lanes(y * chunks + c)],
                W.at[c, pl.ds(pl.multiple_of(y * depth, LANES), depth), pl.ds(k * LANES, LANES)],
                l_w.at[c, k],
            ))
    for i in range(2 * chunks):
        piece = down.at[pl.ds(i * LANES, LANES), :]
        loads.append(pltpu.make_async_copy(piece, d_block(i, b), l_d.at[i]))
        push(piece, d_block(i, b), d_send.at[i], d_recv.at[i], other)
    for load in loads:
        load.start()
    acc[...] = jnp.zeros_like(acc)

    def swap(c, slot, i):
        block = w_share(c, slot, g)
        for e in range(1, G):
            push(block, block, x_send.at[e, c, i], x_recv.at[e, c, i], ((g + e) % G, t, b))

    def from_beside(c):
        for k in range(2):
            got(w_piece(c, 1 - y, k), q_recv.at[c, k])

    def swap_beside(c):
        swap(c, 1 - y, 0)

    def relay(c):
        push(w_share(c, 1 - y, g), w_share(c, 3 - y, g), f_send.at[c], f_recv.at[c], (g, facing, b))

    def from_facing(c):
        for k in range(2):
            got(w_piece(c, 2 + y, k), p_recv.at[c, k])
        swap(c, 2 + y, 1)

    def relayed(c):
        got(w_share(c, 3 - y, g), f_recv.at[c])
        swap(c, 3 - y, 2)

    def pass_tokens(i, k):
        block = x_block(i, b)
        got(block, t_recv.at[k])
        push(block, block, c_send.at[k], c_recv.at[k], other)

    def ready(c):
        for e in range(1, G):
            for i, slot in enumerate((1 - y, 2 + y, 3 - y)):
                got(w_share(c, slot, (g + G - e) % G), x_recv.at[e, c, i])

    def multiply(c, r):
        return jnp.dot(X[r], W[c], preferred_element_type=jnp.float32)

    def keep(c, r):
        Q[c, r] = multiply(c, r)

    def give(c, r):
        S[c, r] = multiply(c, r).astype(S.dtype)
        push(S.at[c, r], R.at[c, r], z_send.at[c, r], z_recv.at[c, r], (g, along, b))

    def h_piece(c, r, k):
        return H.at[y, c, r, :, lanes(k)]

    def finish(c, r):
        got(R.at[c, r], z_recv.at[c, r])
        both = Q[c, r] + R[c, r].astype(jnp.float32)
        hidden = (jax.nn.silu(both[:, :LANES]) * both[:, LANES:]).astype(hs.dtype)
        hs[c, r] = hidden
        block, there = hs.at[c, r], h_piece(c, r, b)
        push(block, there, h_send.at[c, r, 0], h_recv.at[c, r, b], (g, facing, a))
        push(block, there, h_send.at[c, r, 1], h_recv.at[c, r, b], (g, along, a))

        @pl.when(own)
        def _():
            H[y, c, r, :, lanes(b)] = hidden

        @pl.when(foreign)
        def _():
            push(block, there, h_send.at[c, r, 2], h_recv.at[c, r, b], other)

    def onward(c, r):
        push(H.at[y, c, r], H.at[y, c, r], y_send.at[c, r], y_recv.at[c, r], beside)

    def spread_own_inner(c, r):
        got(h_piece(c, r, 1 - b), h_recv.at[c, r, 1 - b])
        onward(c, r)

    def spread_own_outer(c, r):
        for k in range(B):
            got(h_piece(c, r, k), h_recv.at[c, r, k])
        onward(c, r)

    def spread_foreign_inner(c, r):
        for k in range(B):
            got(h_piece(c, r, k), h_recv.at[c, r, k])
        block = H.at[y, c, r]
        push(block, block, r_send.at[c, r], r_recv.at[c, r], (g, along, b))
        onward(c, r)

    def spread_foreign_outer(c, r):
        got(H.at[y, c, r], r_recv.at[c, r])
        onward(c, r)

    def project(c, r):
        got(H.at[1 - y, c, r], y_recv.at[c, r])
        acc[r] += jnp.dot(H[0, c, r], D[c], preferred_element_type=jnp.float32) + jnp.dot(
            H[1, c, r], D[chunks + c], preferred_element_type=jnp.float32
        )

    rz = z % 2

    def pass_beyond():
        block = x_block(beyond, b)
        got(block, t_recv.at[0])
        push(block, block, t_send.at[2], t_recv.at[2], beside)
        push(block, block, c_send.at[0], c_recv.at[0], other)
        for c in range(3, chunks):
            send_beside(c)

    def held(i, k):
        got(x_block(i, 1 - b), c_recv.at[k])

    def settle():
        for load in loads:
            load.wait()

    def settle_down():
        for i in range(2 * chunks):
            got(d_block(i, 1 - b), d_recv.at[i])

    def when(role, stage, *args):
        @pl.when(role)
        def _():
            stage(*args)

    halves = (rz, 1 - rz)
    end = chunks - 1

    def tokens_complete():
        pass_tokens(diagonal, 2)
        held(beyond, 0)
        held(diagonal, 2)

    def each(stage, c, order):
        for r in order:
            stage(c, r)

    @pl.when(inner)
    def _():
        first = (1 - rz, rz)
        from_beside(0)
        relay(0)
        swap_beside(0)
        send_across(2)
        from_facing(0)
        from_facing(1)
        from_beside(1)
        relay(1)
        swap_beside(1)
        relayed(0)
        pass_beyond()
        pass_tokens(near, 1)
        settle()
        held(near, 1)
        ready(0)
        keep(0, rz)
        from_beside(2)
        relay(2)
        tokens_complete()
        from_facing(2)
        keep(0, 1 - rz)
        finish(0, 1 - rz)
        send_across(3)
        when(own, spread_own_inner, 0, 1 - rz)
        relayed(1)
        from_beside(3)
        swap_beside(2)
        finish(0, rz)
        when(own, spread_own_inner, 0, rz)
        settle_down()
        ready(1)
        keep(1, 1 - rz)
        relayed(2)
        when(foreign, spread_foreign_inner, 0, rz)
        finish(1, 1 - rz)
        relay(3)
        when(own, spread_own_inner, 1, 1 - rz)
        keep(1, rz)
        from_facing(3)
        swap_beside(3)
        ready(2)
        keep(2, 1 - rz)
        when(foreign, spread_foreign_inner, 0, 1 - rz)
        finish(1, rz)
        when(own, spread_own_inner, 1, rz)
        keep(2, rz)
        when(foreign, spread_foreign_inner, 1, rz)
        finish(2, 1 - rz)
        relayed(3)
        when(own, spread_own_inner, 2, 1 - rz)
        when(own, each, project, 0, first)
        finish(2, rz)
        when(own, spread_own_inner, 2, rz)
        when(foreign, spread_foreign_inner, 1, 1 - rz)
        when(foreign, spread_foreign_inner, 2, rz)
        ready(3)
        keep(3, 1 - rz)
        when(foreign, spread_foreign_inner, 2, 1 - rz)
        keep(3, rz)

        @pl.when(own)
        def _():
            finish(3, 1 - rz)
            project(1, 1 - rz)
            spread_own_inner(3, 1 - rz)
            finish(3, rz)
            project(1, rz)
            spread_own_inner(3, rz)
            for c in (2, 3):
                each(project, c, first)

        @pl.when(foreign)
        def _():
            each(finish, 3, first)
            spread_foreign_inner(3, rz)
            project(0, rz)
            spread_foreign_inner(3, 1 - rz)
            project(0, 1 - rz)
            for c in (1, 2):
                each(project, c, halves)
            each(project, 3, halves)

    @pl.when(outer)
    def _():
        far = (1 - rz, rz)
        from_beside(0)
        swap_beside(0)
        hear()
        sent(x_block(j, 0), t_send.at[0])
        send_across(0)
        relay(0)
        send_across(1)
        pass_beyond()
        from_beside(1)
        relay(1)
        send_across(2)
        from_facing(0)
        pass_tokens(near, 1)
        relayed(0)
        swap_beside(1)
        from_beside(2)
        relay(2)
        send_across(3)
        from_facing(1)
        settle()
        held(near, 1)
        ready(0)
        give(0, rz)
        relayed(1)
        from_facing(2)
        tokens_complete()
        give(0, 1 - rz)
        swap_beside(2)
        ready(1)
        give(1, rz)
        from_beside(3)
        relay(3)
        relayed(2)
        give(1, 1 - rz)
        from_facing(3)
        swap_beside(3)
        settle_down()
        when(own, spread_own_outer, 0, rz)
        ready(2)
        each(give, 2, halves)
        relayed(3)
        when(own, spread_own_outer, 0, 1 - rz)
        when(own, spread_own_outer, 1, rz)
        when(foreign, spread_foreign_outer, 0, 1 - rz)
        ready(3)
        each(give, 3, halves)

        @pl.when(own)
        def _():
            spread_own_outer(1, 1 - rz)
            each(project, 0, halves)
            for c in (2, 3):
                each(spread_own_outer, c, halves)
                each(project, c - 1, halves)
            each(project, 3, halves)

        @pl.when(foreign)
        def _():
            spread_foreign_outer(0, rz)
            for c in (1, 2, 3):
                each(spread_foreign_outer, c, far)
                each(project, c - 1, far)
            each(project, 3, far)

    for r in range(2):
        out[pl.ds(r * half, half), :] = acc[r].astype(out.dtype)

    when(inner, sent, x_block(j, 0), t_send.at[0])
    for k in range(3):
        if k:
            sent(x_block(j, 0), t_send.at[k])
        sent(x_block(j, 0), c_send.at[k])
    for i in range(2 * chunks):
        sent(d_block(i, b), d_send.at[i])

    def drain(c, carry):
        for k in range(2):
            sent(w_piece(c, 0, k), p_send.at[c, k])
            sent(w_piece(c, 0, k), q_send.at[c, k])
        sent(w_share(c, 0, g), f_send.at[c])
        for e in range(1, G):
            for i in range(3):
                sent(w_share(c, 0, g), x_send.at[e, c, i])
        for r in range(2):
            sent(H.at[y, c, r], y_send.at[c, r])

            @pl.when(outer)
            def _():
                sent(S.at[c, r], z_send.at[c, r])

            @pl.when(inner)
            def _():
                sent(hs.at[c, r], h_send.at[c, r, 0])
                sent(hs.at[c, r], h_send.at[c, r, 1])

            @pl.when(jnp.logical_and(inner, foreign))
            def _():
                sent(hs.at[c, r], h_send.at[c, r, 2])
                sent(H.at[y, c, r], r_send.at[c, r])

        return carry

    lax.fori_loop(0, chunks, drain, 0)


def column_local(G, n, B, tokens, gate_weight, up_weight, down_weight):
    h = n // B
    rows = tokens.shape[0]
    depth, wide = gate_weight.shape
    columns = down_weight.shape[1]
    chunks = wide // LANES // 2
    half = h // 2 * rows
    dtype = tokens.dtype
    DMA = pltpu.SemaphoreType.DMA
    pair = pltpu.VMEM((chunks, 2, half, 2 * LANES), dtype)
    return pl.pallas_call(
        functools.partial(column_layer, G, n, B),
        out_shape=jax.ShapeDtypeStruct((h * rows, columns), dtype),
        in_specs=[ANY] * 4,
        out_specs=pl.BlockSpec(memory_space=pltpu.VMEM),
        scratch_shapes=[
            pltpu.VMEM((2, half, 4 * depth), dtype),
            pltpu.VMEM((chunks, 4 * depth, 2 * LANES), dtype),
            pltpu.VMEM((2 * chunks, B * LANES, columns), dtype),
            pltpu.VMEM((chunks, 2, half, 2 * LANES), jnp.float32),
            pair, pair,
            pltpu.VMEM((chunks, 2, half, LANES), dtype),
            pltpu.VMEM((2, chunks, 2, half, B * LANES), dtype),
            pltpu.VMEM((2, half, columns), jnp.float32),
            DMA((chunks, 2)), DMA((2,)), DMA((2 * chunks,)),
            DMA((chunks, 2)), DMA((chunks, 2)),
            DMA((chunks, 2)), DMA((chunks, 2)),
            DMA((chunks,)), DMA((chunks,)),
            DMA((G, chunks, 3)), DMA((G, chunks, 3)),
            DMA((3,)), DMA((3,)), DMA((3,)), DMA((3,)),
            DMA((2 * chunks,)), DMA((2 * chunks,)),
            DMA((chunks, 2)), DMA((chunks, 2)),
            DMA((chunks, 2, 3)), DMA((chunks, 2, B)),
            DMA((chunks, 2)), DMA((chunks, 2)),
            DMA((chunks, 2)), DMA((chunks, 2)),
            pltpu.SemaphoreType.REGULAR,
        ],
        compiler_params=pltpu.CompilerParams(
            collective_id=0, has_side_effects=True, vmem_limit_bytes=63_000_000
        ),
        name="layer",
    )(tokens, gate_weight, up_weight, down_weight)


def solution(mesh):
    shape = dict(mesh.shape)
    sizes = shape["groups"], shape["tp"], shape["blk"]
    kernel = column_local if sizes[1:] == (8, 2) else local
    return jax.shard_map(
        functools.partial(kernel, *sizes),
        mesh=mesh,
        in_specs=(P(("groups", "tp"), None), P("tp", "blk"), P("tp", "blk"), P("blk", "tp")),
        out_specs=P(("groups", "blk"), "tp"),
        check_vma=False,
    )
```

```python
import functools

import jax
import jax.numpy as jnp
from jax import lax
from jax.experimental import pallas as pl
from jax.experimental.pallas import tpu as pltpu
from jax.sharding import PartitionSpec as P

MESH = pl.DeviceIdType.MESH
ANY = pl.BlockSpec(memory_space=pl.ANY)


def flip1(i):
    return i + 1 - 2 * (i % 2)


def greet(devices):
    barrier = pltpu.get_barrier_semaphore()
    for device in devices:
        pl.semaphore_signal(barrier, inc=1, device_id=device, device_id_type=MESH)
    pl.semaphore_wait(barrier, len(devices))


def flip2(i):
    return i + 2 - 4 * ((i // 2) % 2)


CUT = 8


def layer(
    G, n, B,
    tok, gate, up, down, out,
    T, W, D, both, mine_h, H, total,
    lsem, tok_send, tok_recv, core_send, core_recv,
    w_send, w_recv, x_send, x_recv, d_send, d_recv,
    h_send, h_recv, f_send, f_recv,
):
    g, t, b = lax.axis_index("groups"), lax.axis_index("tp"), lax.axis_index("blk")
    h = n // B
    a, j = t // h, t % h
    half, pairs = h // 2, n // 2
    p, y = t // 2, t % 2
    other = (g, t, 1 - b)
    across = (g, flip1(t), b)
    R, K = tok.shape
    width = K // B
    depth, units = gate.shape[0], gate.shape[1] // h
    part = depth // G
    mine = pl.ds(pl.multiple_of(b * width, 128), width)
    theirs = pl.ds(pl.multiple_of((1 - b) * width, 128), width)
    square = h == 4
    cut = R * CUT // 16
    upper, lower_rows = pl.ds(0, cut), pl.ds(cut, R - cut)

    greet(
        [(g, (t + d) % n, b) for d in range(1, n)]
        + [(g, 2 * ((p + d) % pairs) + y, 1 - b) for d in range(1, pairs)]
        + [((g + e) % G, t, b) for e in range(1, G)]
        + [other]
    )

    def remote(src, dst, send, recv, device):
        return pltpu.make_async_remote_copy(
            src_ref=src, dst_ref=dst, send_sem=send, recv_sem=recv,
            device_id=device, device_id_type=MESH,
        )

    pending = []

    def push(*copy):
        c = remote(*copy)
        c.start()
        pending.append(c)

    def local(src, dst, sem):
        return pltpu.make_async_copy(src, dst, sem)

    def rows_of(i, s):
        if square:
            i = flip1(i) if s % 2 else i
            return flip2(i) if s // 2 else i
        return (i + h - s) % h

    def token_block(s):
        return T.at[rows_of(j, s), :, mine]

    def w_block(source, first, size, k):
        start = pl.multiple_of(source * depth + first, 16)
        return W.at[pl.ds(start, size), pl.ds(k * units, units)]

    own_columns = pl.ds(pl.multiple_of(j * units, 128), units)
    loads = [
        local(gate.at[:, own_columns], w_block(t, 0, depth, 0), lsem.at[0]),
        local(up.at[:, own_columns], w_block(t, 0, depth, 1), lsem.at[1]),
        local(tok, T.at[j], lsem.at[2]),
        local(down, D.at[b], lsem.at[3]),
    ]

    first = g * part
    rows = pl.ds(pl.multiple_of(first, 16), part)
    order = [d for k in range(1, n // 2) for d in (k, n - k)] + [n // 2]
    for d in order:
        dest = (t + d) % n
        cols = pl.ds(pl.multiple_of((dest % h) * units, 128), units)
        for k in range(2):
            push(
                (gate, up)[k].at[rows, cols], w_block(t, first, part, k),
                w_send.at[d, k], w_recv.at[d, k], (g, dest, b),
            )

    for s in (2, 1) if square else range(1, h):
        dest = rows_of(j, s) if square else (j + s) % h
        push(tok.at[:, mine], T.at[j, :, mine], tok_send.at[s], tok_recv.at[s], (g, a * h + dest, b))
    push(down, D.at[b], d_send, d_recv, other)
    for load in loads:
        load.start()

    for d in order:
        source = (t + n - d) % n
        for k in range(2):
            block = w_block(source, first, part, k)
            remote(block, block, w_send.at[d, k], w_recv.at[d, k], other).wait_recv()
            for e in range(1, G):
                push(block, block, x_send.at[e, d, k], x_recv.at[e, d, k], ((g + e) % G, t, b))
    for load in loads:
        load.wait()
    remote(D.at[1 - b], D.at[1 - b], d_send, d_recv, other).wait_recv()
    total[...] = jnp.zeros_like(total)

    def tokens_arrive(s):
        block = token_block(s)
        if square and s == 3:
            for i, r in ((3, upper), (0, lower_rows)):
                piece = T.at[rows_of(j, s), r, mine]
                remote(piece, piece, tok_send.at[i], tok_recv.at[i], other).wait_recv()
        else:
            remote(block, block, tok_send.at[s], tok_recv.at[s], other).wait_recv()
        if square and s < 3:
            piece = T.at[rows_of(j, s), (upper, lower_rows)[s - 1], mine]
            target = flip2(j) if s == 1 else flip1(j)
            i = 3 if s == 1 else 0
            push(piece, piece, tok_send.at[i], tok_recv.at[i], (g, a * h + target, b))

        push(block, block, core_send.at[s], core_recv.at[s], other)

    def compute(s):
        slot = rows_of(j, s)
        if s > 0:
            block = T.at[slot, :, theirs]
            remote(block, block, core_send.at[s], core_recv.at[s], other).wait_recv()
        tiles = 4 if K % 512 == 0 else 1
        tile = K // tiles
        both[...] = jnp.zeros_like(both)

        def body(i, carry):
            k = pl.ds(pl.multiple_of(i * tile, 128), tile)
            both[...] += jnp.dot(T[slot, :, k], W[k, :], preferred_element_type=jnp.float32)
            return carry

        lax.fori_loop(0, tiles, body, 0)
        hidden = (jax.nn.silu(both[:, :units]) * both[:, units:]).astype(out.dtype)
        mine_h[s] = hidden

        @pl.when(a == b)
        def _():
            H[s, j, b] = hidden

        for d in sorted(range(1, pairs), key=lambda d: min(d, pairs - d)):
            push(
                mine_h.at[s], H.at[s, j, b], h_send.at[s, d], h_recv.at[s, j // 2, b],
                (g, 2 * ((p + d) % pairs) + y, a),
            )

        @pl.when(a != b)
        def _():
            remote(mine_h.at[s], H.at[s, j, b], h_send.at[s, 0], h_recv.at[s, j // 2, b], other).start()

    def pass_on(s):
        for k in range(half):
            for c in range(B):
                block = H.at[s, 2 * k + y, c]

                @pl.when(jnp.logical_not((a == b) & (j // 2 == k) & (c == b)))
                def _():
                    remote(block, block, h_send.at[s, 0], h_recv.at[s, k, c], other).wait_recv()

                push(block, block, f_send.at[s, k, c], f_recv.at[s, k, c], across)

    def lower(s):
        for k in range(half):
            for c in range(B):
                block = H.at[s, 2 * k + 1 - y, c]
                remote(block, block, f_send.at[s, k, c], f_recv.at[s, k, c], across).wait_recv()

        def body(i, carry):
            r = rows_of(i, s)
            term = total[r]
            for c in range(B):
                term += jnp.dot(
                    H[s, i, c], D[c, pl.ds(pl.multiple_of(i * units, 128), units), :],
                    preferred_element_type=jnp.float32,
                )
            total[r] = term
            return carry

        lax.fori_loop(0, h, body, 0)

    for d in order:
        source = (t + n - d) % n
        for e in range(1, G):
            for k in range(2):
                block = w_block(source, ((g + G - e) % G) * part, part, k)
                remote(block, block, x_send.at[e, d, k], x_recv.at[e, d, k], other).wait_recv()

    compute(0)
    for s in range(1, h):
        tokens_arrive(s)
        compute(s)
        pass_on(s - 1)
        if s >= 2:
            lower(s - 2)
    pass_on(h - 1)
    lower(h - 2)
    lower(h - 1)
    for r in range(h):
        out[pl.ds(r * R, R), :] = total[r].astype(out.dtype)

    for c in pending:
        c.wait_send()
    @pl.when(a != b)
    def _():
        for s in range(h):
            remote(mine_h.at[s], mine_h.at[s], h_send.at[s, 0], h_recv.at[s, 0, 0], other).wait_send()


def local(G, n, B, tokens, gate_weight, up_weight, down_weight):
    h = n // B
    R, K = tokens.shape
    depth, wide = gate_weight.shape
    units, columns = wide // h, down_weight.shape[1]
    dtype = tokens.dtype
    DMA = pltpu.SemaphoreType.DMA
    return pl.pallas_call(
        functools.partial(layer, G, n, B),
        out_shape=jax.ShapeDtypeStruct((h * R, columns), dtype),
        in_specs=[ANY] * 4,
        out_specs=pl.BlockSpec(memory_space=pltpu.VMEM),
        scratch_shapes=[
            pltpu.VMEM((h, R, K), dtype),
            pltpu.VMEM((K, 2 * units), dtype),
            pltpu.VMEM((B, wide, columns), dtype),
            pltpu.VMEM((R, 2 * units), jnp.float32),
            pltpu.VMEM((h, R, units), dtype),
            pltpu.VMEM((h, h, B, R, units), dtype),
            pltpu.VMEM((h, R, columns), jnp.float32),
            DMA((4,)),
            DMA((h,)), DMA((h,)), DMA((h,)), DMA((h,)),
            DMA((n, 2)), DMA((n, 2)),
            DMA((G, n, 2)), DMA((G, n, 2)),
            DMA, DMA,
            DMA((h, n // 2)), DMA((h, h // 2, B)),
            DMA((h, h // 2, B)), DMA((h, h // 2, B)),
        ],
        compiler_params=pltpu.CompilerParams(
            collective_id=0, has_side_effects=True, vmem_limit_bytes=63_000_000
        ),
        name="layer",
    )(tokens, gate_weight, up_weight, down_weight)


LANES = 128


def column_layer(
    G, n, B,
    tok, gate, up, down, out,
    X, W, D, Q, S, R, hs, H, acc,
    l_w, l_x, l_d,
    p_send, p_recv, q_send, q_recv, f_send, f_recv, x_send, x_recv,
    t_send, t_recv, c_send, c_recv, d_send, d_recv,
    z_send, z_recv, h_send, h_recv, r_send, r_recv, y_send, y_recv, word,
):
    g, t, b = lax.axis_index("groups"), lax.axis_index("tp"), lax.axis_index("blk")
    h = n // B
    z, y, j, a = t // 2, t % 2, t % h, t // h
    last = n // 2 - 1
    mz = last - z
    inner = z % 2 + a == 1
    outer = z % 2 + a != 1
    own, foreign = b == a, b != a
    rows, depth, wide = tok.shape[0], gate.shape[0], gate.shape[1]
    part, run, half = depth // G, 2 * depth, h // 2 * rows
    chunks = wide // LANES // 2
    other = (g, t, 1 - b)
    beside = (g, flip1(t), b)
    along = flip2(t)
    facing = 2 * mz + y

    near_by = [(g, along, c) for c in range(B)] + [other, beside]
    near_by += [((g + e) % G, t, b) for e in range(1, G)]
    opposite = [(g, facing, c) for c in range(B)]

    @pl.when(inner)
    def _():
        greet(near_by + opposite)

    @pl.when(outer)
    def _():
        greet(near_by)

    def tell(device):
        pl.semaphore_signal(word, inc=1, device_id=device, device_id_type=MESH)

    def hear():
        pl.semaphore_wait(word, 1)

    def remote(src, dst, send, recv, device):
        return pltpu.make_async_remote_copy(
            src_ref=src, dst_ref=dst, send_sem=send, recv_sem=recv,
            device_id=device, device_id_type=MESH,
        )

    def push(*copy):
        remote(*copy).start()

    def got(ref, sem):
        remote(ref, ref, sem, sem, other).wait_recv()

    def sent(ref, sem):
        remote(ref, ref, sem, sem, other).wait_send()

    def lanes(k):
        return pl.ds(pl.multiple_of(k * LANES, LANES), LANES)

    share = pl.ds(pl.multiple_of(g * part, 16), part)

    def landing(k, e):
        return pl.ds(pl.multiple_of(k * depth + e * part, 16), part)

    def w_piece(c, slot, k):
        return W.at[c, landing(slot, g), pl.ds(k * LANES, LANES)]

    def w_share(c, slot, e):
        return W.at[c, landing(slot, e), :]

    def depth_of(row):
        return pl.ds(pl.multiple_of(row * run, LANES), run)

    def x_block(i, k):
        return X.at[
            i // 2, pl.ds(pl.multiple_of(i % 2 * rows, 16), rows),
            pl.ds(pl.multiple_of(k * run, LANES), run),
        ]

    def d_block(i, k):
        return D.at[i, pl.ds(pl.multiple_of(k * LANES, LANES), LANES), :]

    near, beyond, diagonal = flip1(j), flip2(j), flip1(flip2(j))
    z2 = along // 2
    row_there = z2 + b * (last - 2 * z2)
    row_here = z + b * (mz - z)

    def send_across(c):
        for k in range(2):
            push(
                (gate, up)[k].at[share, lanes(y * chunks + c)], w_piece(c, 2 + y, k),
                p_send.at[c, k], p_recv.at[c, k], (g, facing, b),
            )

    def send_beside(c):
        for k in range(2):
            push(
                (gate, up)[k].at[share, lanes((1 - y) * chunks + c)], w_piece(c, y, k),
                q_send.at[c, k], q_recv.at[c, k], beside,
            )

    push(tok.at[:, depth_of(row_there)], x_block(j, b), t_send.at[0], t_recv.at[0], (g, along, b))
    send_beside(0)
    send_beside(1)
    push(tok.at[:, depth_of(row_here)], x_block(j, b), t_send.at[1], t_recv.at[1], beside)
    send_beside(2)

    @pl.when(inner)
    def _():
        send_across(0)
        send_across(1)
        tell((g, facing, b))
        hear()
        tell((g, along, b))

    loads = []
    for k, row in enumerate((z, mz)):
        loads.append(pltpu.make_async_copy(tok.at[:, depth_of(row)], x_block(j, k), l_x.at[k]))
    for c in range(chunks):
        for k in range(2):
            loads.append(pltpu.make_async_copy(
                (gate, up)[k].at[:, lanes(y * chunks + c)],
                W.at[c, pl.ds(pl.multiple_of(y * depth, LANES), depth), pl.ds(k * LANES, LANES)],
                l_w.at[c, k],
            ))
    for i in range(2 * chunks):
        piece = down.at[pl.ds(i * LANES, LANES), :]
        loads.append(pltpu.make_async_copy(piece, d_block(i, b), l_d.at[i]))
        push(piece, d_block(i, b), d_send.at[i], d_recv.at[i], other)
    for load in loads:
        load.start()
    acc[...] = jnp.zeros_like(acc)

    def swap(c, slot, i):
        block = w_share(c, slot, g)
        for e in range(1, G):
            push(block, block, x_send.at[e, c, i], x_recv.at[e, c, i], ((g + e) % G, t, b))

    def from_beside(c):
        for k in range(2):
            got(w_piece(c, 1 - y, k), q_recv.at[c, k])

    def swap_beside(c):
        swap(c, 1 - y, 0)

    def relay(c):
        push(w_share(c, 1 - y, g), w_share(c, 3 - y, g), f_send.at[c], f_recv.at[c], (g, facing, b))

    def from_facing(c):
        for k in range(2):
            got(w_piece(c, 2 + y, k), p_recv.at[c, k])
        swap(c, 2 + y, 1)

    def relayed(c):
        got(w_share(c, 3 - y, g), f_recv.at[c])
        swap(c, 3 - y, 2)

    def pass_tokens(i, k):
        block = x_block(i, b)
        got(block, t_recv.at[k])
        push(block, block, c_send.at[k], c_recv.at[k], other)

    def ready(c):
        for e in range(1, G):
            for i, slot in enumerate((1 - y, 2 + y, 3 - y)):
                got(w_share(c, slot, (g + G - e) % G), x_recv.at[e, c, i])

    def multiply(c, r):
        return jnp.dot(X[r], W[c], preferred_element_type=jnp.float32)

    def keep(c, r):
        Q[c, r] = multiply(c, r)

    def give(c, r):
        S[c, r] = multiply(c, r).astype(S.dtype)
        push(S.at[c, r], R.at[c, r], z_send.at[c, r], z_recv.at[c, r], (g, along, b))

    def h_piece(c, r, k):
        return H.at[y, c, r, :, lanes(k)]

    def finish(c, r):
        got(R.at[c, r], z_recv.at[c, r])
        both = Q[c, r] + R[c, r].astype(jnp.float32)
        hidden = (jax.nn.silu(both[:, :LANES]) * both[:, LANES:]).astype(hs.dtype)
        hs[c, r] = hidden
        block, there = hs.at[c, r], h_piece(c, r, b)
        push(block, there, h_send.at[c, r, 0], h_recv.at[c, r, b], (g, facing, a))
        push(block, there, h_send.at[c, r, 1], h_recv.at[c, r, b], (g, along, a))

        @pl.when(own)
        def _():
            H[y, c, r, :, lanes(b)] = hidden

        @pl.when(foreign)
        def _():
            push(block, there, h_send.at[c, r, 2], h_recv.at[c, r, b], other)

    def onward(c, r):
        push(H.at[y, c, r], H.at[y, c, r], y_send.at[c, r], y_recv.at[c, r], beside)

    def spread_own_inner(c, r):
        got(h_piece(c, r, 1 - b), h_recv.at[c, r, 1 - b])
        onward(c, r)

    def spread_own_outer(c, r):
        for k in range(B):
            got(h_piece(c, r, k), h_recv.at[c, r, k])
        onward(c, r)

    def spread_foreign_inner(c, r):
        for k in range(B):
            got(h_piece(c, r, k), h_recv.at[c, r, k])
        block = H.at[y, c, r]
        push(block, block, r_send.at[c, r], r_recv.at[c, r], (g, along, b))
        onward(c, r)

    def spread_foreign_outer(c, r):
        got(H.at[y, c, r], r_recv.at[c, r])
        onward(c, r)

    def term(c, r):
        got(H.at[1 - y, c, r], y_recv.at[c, r])
        return jnp.dot(H[0, c, r], D[c], preferred_element_type=jnp.float32) + jnp.dot(
            H[1, c, r], D[chunks + c], preferred_element_type=jnp.float32
        )

    def project(c, r):
        acc[r] += term(c, r)

    def deliver(c, r):
        out[pl.ds(pl.multiple_of(r * half, 16), half), :] = (acc[r] + term(c, r)).astype(out.dtype)

    rz = z % 2

    def pass_beyond():
        block = x_block(beyond, b)
        got(block, t_recv.at[0])
        push(block, block, t_send.at[2], t_recv.at[2], beside)
        push(block, block, c_send.at[0], c_recv.at[0], other)
        for c in range(3, chunks):
            send_beside(c)

    def held(i, k):
        got(x_block(i, 1 - b), c_recv.at[k])

    def settle():
        for load in loads:
            load.wait()

    def settle_down():
        for i in range(2 * chunks):
            got(d_block(i, 1 - b), d_recv.at[i])

    def when(role, stage, *args):
        @pl.when(role)
        def _():
            stage(*args)

    halves = (rz, 1 - rz)
    end = chunks - 1

    def tokens_complete():
        pass_tokens(diagonal, 2)
        held(beyond, 0)
        held(diagonal, 2)

    def each(stage, c, order):
        for r in order:
            stage(c, r)

    @pl.when(inner)
    def _():
        first = (1 - rz, rz)
        from_beside(0)
        relay(0)
        swap_beside(0)
        send_across(2)
        from_facing(0)
        from_facing(1)
        from_beside(1)
        relay(1)
        swap_beside(1)
        relayed(0)
        pass_beyond()
        pass_tokens(near, 1)
        settle()
        held(near, 1)
        ready(0)
        keep(0, rz)
        from_beside(2)
        relay(2)
        tokens_complete()
        from_facing(2)
        keep(0, 1 - rz)
        finish(0, 1 - rz)
        when(own, spread_own_inner, 0, 1 - rz)
        relayed(1)
        from_beside(3)
        swap_beside(2)
        finish(0, rz)
        send_across(3)
        when(own, spread_own_inner, 0, rz)
        settle_down()
        when(foreign, spread_foreign_inner, 0, rz)
        ready(1)
        keep(1, 1 - rz)
        relayed(2)
        finish(1, 1 - rz)
        relay(3)
        when(own, spread_own_inner, 1, 1 - rz)
        when(foreign, spread_foreign_inner, 0, 1 - rz)
        keep(1, rz)
        from_facing(3)
        swap_beside(3)
        ready(2)
        keep(2, 1 - rz)
        finish(1, rz)
        when(own, spread_own_inner, 1, rz)
        when(foreign, spread_foreign_inner, 1, rz)
        keep(2, rz)
        finish(2, 1 - rz)
        relayed(3)
        when(own, spread_own_inner, 2, 1 - rz)
        when(own, each, project, 0, first)
        finish(2, rz)
        when(own, spread_own_inner, 2, rz)
        when(foreign, spread_foreign_inner, 1, 1 - rz)
        when(foreign, spread_foreign_inner, 2, rz)
        ready(3)
        keep(3, 1 - rz)
        when(foreign, spread_foreign_inner, 2, 1 - rz)
        keep(3, rz)

        @pl.when(own)
        def _():
            finish(3, 1 - rz)
            project(1, 1 - rz)
            spread_own_inner(3, 1 - rz)
            finish(3, rz)
            project(1, rz)
            spread_own_inner(3, rz)
            each(project, 2, first)
            each(deliver, 3, first)

        @pl.when(foreign)
        def _():
            each(finish, 3, first)
            spread_foreign_inner(3, rz)
            project(0, rz)
            spread_foreign_inner(3, 1 - rz)
            project(0, 1 - rz)
            for c in (1, 2):
                each(project, c, halves)
            each(deliver, 3, halves)

    @pl.when(outer)
    def _():
        far = (1 - rz, rz)
        from_beside(0)
        swap_beside(0)
        hear()
        sent(x_block(j, 0), t_send.at[0])
        send_across(0)
        relay(0)
        send_across(1)
        pass_beyond()
        from_beside(1)
        relay(1)
        send_across(2)
        from_facing(0)
        pass_tokens(near, 1)
        relayed(0)
        swap_beside(1)
        from_beside(2)
        relay(2)
        send_across(3)
        from_facing(1)
        settle()
        held(near, 1)
        ready(0)
        give(0, rz)
        relayed(1)
        from_facing(2)
        tokens_complete()
        give(0, 1 - rz)
        swap_beside(2)
        ready(1)
        give(1, rz)
        from_beside(3)
        relay(3)
        relayed(2)
        give(1, 1 - rz)
        from_facing(3)
        swap_beside(3)
        settle_down()
        when(own, spread_own_outer, 0, rz)
        ready(2)
        each(give, 2, halves)
        when(foreign, spread_foreign_outer, 0, 1 - rz)
        when(own, spread_own_outer, 0, 1 - rz)
        relayed(3)
        ready(3)
        when(own, spread_own_outer, 1, rz)
        when(foreign, spread_foreign_outer, 0, rz)
        give(3, rz)
        when(own, spread_own_outer, 1, 1 - rz)
        give(3, 1 - rz)

        @pl.when(own)
        def _():
            spread_own_outer(2, rz)
            each(project, 0, halves)
            spread_own_outer(2, 1 - rz)
            each(project, 1, halves)
            each(spread_own_outer, 3, halves)
            each(project, 2, halves)
            each(deliver, 3, halves)

        @pl.when(foreign)
        def _():
            for c in (1, 2, 3):
                each(spread_foreign_outer, c, far)
                each(project, c - 1, far)
            each(deliver, 3, far)

    when(inner, sent, x_block(j, 0), t_send.at[0])
    for k in range(3):
        if k:
            sent(x_block(j, 0), t_send.at[k])
        sent(x_block(j, 0), c_send.at[k])
    for i in range(2 * chunks):
        sent(d_block(i, b), d_send.at[i])

    def drain(c, carry):
        for k in range(2):
            sent(w_piece(c, 0, k), p_send.at[c, k])
            sent(w_piece(c, 0, k), q_send.at[c, k])
        sent(w_share(c, 0, g), f_send.at[c])
        for e in range(1, G):
            for i in range(3):
                sent(w_share(c, 0, g), x_send.at[e, c, i])
        for r in range(2):
            sent(H.at[y, c, r], y_send.at[c, r])

            @pl.when(outer)
            def _():
                sent(S.at[c, r], z_send.at[c, r])

            @pl.when(inner)
            def _():
                sent(hs.at[c, r], h_send.at[c, r, 0])
                sent(hs.at[c, r], h_send.at[c, r, 1])

            @pl.when(jnp.logical_and(inner, foreign))
            def _():
                sent(hs.at[c, r], h_send.at[c, r, 2])
                sent(H.at[y, c, r], r_send.at[c, r])

        return carry

    lax.fori_loop(0, chunks, drain, 0)


def column_local(G, n, B, tokens, gate_weight, up_weight, down_weight):
    h = n // B
    rows = tokens.shape[0]
    depth, wide = gate_weight.shape
    columns = down_weight.shape[1]
    chunks = wide // LANES // 2
    half = h // 2 * rows
    dtype = tokens.dtype
    DMA = pltpu.SemaphoreType.DMA
    pair = pltpu.VMEM((chunks, 2, half, 2 * LANES), dtype)
    return pl.pallas_call(
        functools.partial(column_layer, G, n, B),
        out_shape=jax.ShapeDtypeStruct((h * rows, columns), dtype),
        in_specs=[ANY] * 4,
        out_specs=pl.BlockSpec(memory_space=pltpu.VMEM),
        scratch_shapes=[
            pltpu.VMEM((2, half, 4 * depth), dtype),
            pltpu.VMEM((chunks, 4 * depth, 2 * LANES), dtype),
            pltpu.VMEM((2 * chunks, B * LANES, columns), dtype),
            pltpu.VMEM((chunks, 2, half, 2 * LANES), jnp.float32),
            pair, pair,
            pltpu.VMEM((chunks, 2, half, LANES), dtype),
            pltpu.VMEM((2, chunks, 2, half, B * LANES), dtype),
            pltpu.VMEM((2, half, columns), jnp.float32),
            DMA((chunks, 2)), DMA((2,)), DMA((2 * chunks,)),
            DMA((chunks, 2)), DMA((chunks, 2)),
            DMA((chunks, 2)), DMA((chunks, 2)),
            DMA((chunks,)), DMA((chunks,)),
            DMA((G, chunks, 3)), DMA((G, chunks, 3)),
            DMA((3,)), DMA((3,)), DMA((3,)), DMA((3,)),
            DMA((2 * chunks,)), DMA((2 * chunks,)),
            DMA((chunks, 2)), DMA((chunks, 2)),
            DMA((chunks, 2, 3)), DMA((chunks, 2, B)),
            DMA((chunks, 2)), DMA((chunks, 2)),
            DMA((chunks, 2)), DMA((chunks, 2)),
            pltpu.SemaphoreType.REGULAR,
        ],
        compiler_params=pltpu.CompilerParams(
            collective_id=0, has_side_effects=True, vmem_limit_bytes=54_000_000
        ),
        name="layer",
    )(tokens, gate_weight, up_weight, down_weight)


def solution(mesh):
    shape = dict(mesh.shape)
    sizes = shape["groups"], shape["tp"], shape["blk"]
    kernel = column_local if sizes[1:] == (8, 2) else local
    return jax.shard_map(
        functools.partial(kernel, *sizes),
        mesh=mesh,
        in_specs=(P(("groups", "tp"), None), P("tp", "blk"), P("tp", "blk"), P("blk", "tp")),
        out_specs=P(("groups", "blk"), "tp"),
        check_vma=False,
    )
```

```python
import functools

import jax
import jax.numpy as jnp
from jax import lax
from jax.experimental import pallas as pl
from jax.experimental.pallas import tpu as pltpu
from jax.sharding import PartitionSpec as P

MESH = pl.DeviceIdType.MESH
ANY = pl.BlockSpec(memory_space=pl.ANY)


def flip1(i):
    return i + 1 - 2 * (i % 2)


def greet(devices):
    barrier = pltpu.get_barrier_semaphore()
    for device in devices:
        pl.semaphore_signal(barrier, inc=1, device_id=device, device_id_type=MESH)
    pl.semaphore_wait(barrier, len(devices))


def flip2(i):
    return i + 2 - 4 * ((i // 2) % 2)


CUT = 8


def layer(
    G, n, B,
    tok, gate, up, down, out,
    T, W, D, both, mine_h, H, total,
    lsem, tok_send, tok_recv, core_send, core_recv,
    w_send, w_recv, x_send, x_recv, d_send, d_recv,
    h_send, h_recv, f_send, f_recv,
):
    g, t, b = lax.axis_index("groups"), lax.axis_index("tp"), lax.axis_index("blk")
    h = n // B
    a, j = t // h, t % h
    half, pairs = h // 2, n // 2
    p, y = t // 2, t % 2
    other = (g, t, 1 - b)
    across = (g, flip1(t), b)
    R, K = tok.shape
    width = K // B
    depth, units = gate.shape[0], gate.shape[1] // h
    part = depth // G
    mine = pl.ds(pl.multiple_of(b * width, 128), width)
    theirs = pl.ds(pl.multiple_of((1 - b) * width, 128), width)
    square = h == 4
    cut = R * CUT // 16
    upper, lower_rows = pl.ds(0, cut), pl.ds(cut, R - cut)

    greet(
        [(g, (t + d) % n, b) for d in range(1, n)]
        + [(g, 2 * ((p + d) % pairs) + y, 1 - b) for d in range(1, pairs)]
        + [((g + e) % G, t, b) for e in range(1, G)]
        + [other]
    )

    def remote(src, dst, send, recv, device):
        return pltpu.make_async_remote_copy(
            src_ref=src, dst_ref=dst, send_sem=send, recv_sem=recv,
            device_id=device, device_id_type=MESH,
        )

    pending = []

    def push(*copy):
        c = remote(*copy)
        c.start()
        pending.append(c)

    def local(src, dst, sem):
        return pltpu.make_async_copy(src, dst, sem)

    def rows_of(i, s):
        if square:
            i = flip1(i) if s % 2 else i
            return flip2(i) if s // 2 else i
        return (i + h - s) % h

    def token_block(s):
        return T.at[rows_of(j, s), :, mine]

    def w_block(source, first, size, k):
        start = pl.multiple_of(source * depth + first, 16)
        return W.at[pl.ds(start, size), pl.ds(k * units, units)]

    own_columns = pl.ds(pl.multiple_of(j * units, 128), units)
    loads = [
        local(gate.at[:, own_columns], w_block(t, 0, depth, 0), lsem.at[0]),
        local(up.at[:, own_columns], w_block(t, 0, depth, 1), lsem.at[1]),
        local(tok, T.at[j], lsem.at[2]),
        local(down, D.at[b], lsem.at[3]),
    ]

    first = g * part
    rows = pl.ds(pl.multiple_of(first, 16), part)
    order = [d for k in range(1, n // 2) for d in (k, n - k)] + [n // 2]
    for d in order:
        dest = (t + d) % n
        cols = pl.ds(pl.multiple_of((dest % h) * units, 128), units)
        for k in range(2):
            push(
                (gate, up)[k].at[rows, cols], w_block(t, first, part, k),
                w_send.at[d, k], w_recv.at[d, k], (g, dest, b),
            )

    for s in (2, 1) if square else range(1, h):
        dest = rows_of(j, s) if square else (j + s) % h
        push(tok.at[:, mine], T.at[j, :, mine], tok_send.at[s], tok_recv.at[s], (g, a * h + dest, b))
    push(down, D.at[b], d_send, d_recv, other)
    for load in loads:
        load.start()

    for d in order:
        source = (t + n - d) % n
        for k in range(2):
            block = w_block(source, first, part, k)
            remote(block, block, w_send.at[d, k], w_recv.at[d, k], other).wait_recv()
            for e in range(1, G):
                push(block, block, x_send.at[e, d, k], x_recv.at[e, d, k], ((g + e) % G, t, b))
    for load in loads:
        load.wait()
    remote(D.at[1 - b], D.at[1 - b], d_send, d_recv, other).wait_recv()
    total[...] = jnp.zeros_like(total)

    def tokens_arrive(s):
        block = token_block(s)
        if square and s == 3:
            for i, r in ((3, upper), (0, lower_rows)):
                piece = T.at[rows_of(j, s), r, mine]
                remote(piece, piece, tok_send.at[i], tok_recv.at[i], other).wait_recv()
        else:
            remote(block, block, tok_send.at[s], tok_recv.at[s], other).wait_recv()
        if square and s < 3:
            piece = T.at[rows_of(j, s), (upper, lower_rows)[s - 1], mine]
            target = flip2(j) if s == 1 else flip1(j)
            i = 3 if s == 1 else 0
            push(piece, piece, tok_send.at[i], tok_recv.at[i], (g, a * h + target, b))

        push(block, block, core_send.at[s], core_recv.at[s], other)

    def compute(s):
        slot = rows_of(j, s)
        if s > 0:
            block = T.at[slot, :, theirs]
            remote(block, block, core_send.at[s], core_recv.at[s], other).wait_recv()
        tiles = 4 if K % 512 == 0 else 1
        tile = K // tiles
        both[...] = jnp.zeros_like(both)

        def body(i, carry):
            k = pl.ds(pl.multiple_of(i * tile, 128), tile)
            both[...] += jnp.dot(T[slot, :, k], W[k, :], preferred_element_type=jnp.float32)
            return carry

        lax.fori_loop(0, tiles, body, 0)
        hidden = (jax.nn.silu(both[:, :units]) * both[:, units:]).astype(out.dtype)
        mine_h[s] = hidden

        @pl.when(a == b)
        def _():
            H[s, j, b] = hidden

        for d in sorted(range(1, pairs), key=lambda d: min(d, pairs - d)):
            push(
                mine_h.at[s], H.at[s, j, b], h_send.at[s, d], h_recv.at[s, j // 2, b],
                (g, 2 * ((p + d) % pairs) + y, a),
            )

        @pl.when(a != b)
        def _():
            remote(mine_h.at[s], H.at[s, j, b], h_send.at[s, 0], h_recv.at[s, j // 2, b], other).start()

    def pass_on(s):
        for k in range(half):
            for c in range(B):
                block = H.at[s, 2 * k + y, c]

                @pl.when(jnp.logical_not((a == b) & (j // 2 == k) & (c == b)))
                def _():
                    remote(block, block, h_send.at[s, 0], h_recv.at[s, k, c], other).wait_recv()

                push(block, block, f_send.at[s, k, c], f_recv.at[s, k, c], across)

    def lower(s):
        for k in range(half):
            for c in range(B):
                block = H.at[s, 2 * k + 1 - y, c]
                remote(block, block, f_send.at[s, k, c], f_recv.at[s, k, c], across).wait_recv()

        def body(i, carry):
            r = rows_of(i, s)
            term = total[r]
            for c in range(B):
                term += jnp.dot(
                    H[s, i, c], D[c, pl.ds(pl.multiple_of(i * units, 128), units), :],
                    preferred_element_type=jnp.float32,
                )
            total[r] = term
            return carry

        lax.fori_loop(0, h, body, 0)

    for d in order:
        source = (t + n - d) % n
        for e in range(1, G):
            for k in range(2):
                block = w_block(source, ((g + G - e) % G) * part, part, k)
                remote(block, block, x_send.at[e, d, k], x_recv.at[e, d, k], other).wait_recv()

    compute(0)
    for s in range(1, h):
        tokens_arrive(s)
        compute(s)
        pass_on(s - 1)
        if s >= 2:
            lower(s - 2)
    pass_on(h - 1)
    lower(h - 2)
    lower(h - 1)
    for r in range(h):
        out[pl.ds(r * R, R), :] = total[r].astype(out.dtype)

    for c in pending:
        c.wait_send()
    @pl.when(a != b)
    def _():
        for s in range(h):
            remote(mine_h.at[s], mine_h.at[s], h_send.at[s, 0], h_recv.at[s, 0, 0], other).wait_send()


def local(G, n, B, tokens, gate_weight, up_weight, down_weight):
    h = n // B
    R, K = tokens.shape
    depth, wide = gate_weight.shape
    units, columns = wide // h, down_weight.shape[1]
    dtype = tokens.dtype
    DMA = pltpu.SemaphoreType.DMA
    return pl.pallas_call(
        functools.partial(layer, G, n, B),
        out_shape=jax.ShapeDtypeStruct((h * R, columns), dtype),
        in_specs=[ANY] * 4,
        out_specs=pl.BlockSpec(memory_space=pltpu.VMEM),
        scratch_shapes=[
            pltpu.VMEM((h, R, K), dtype),
            pltpu.VMEM((K, 2 * units), dtype),
            pltpu.VMEM((B, wide, columns), dtype),
            pltpu.VMEM((R, 2 * units), jnp.float32),
            pltpu.VMEM((h, R, units), dtype),
            pltpu.VMEM((h, h, B, R, units), dtype),
            pltpu.VMEM((h, R, columns), jnp.float32),
            DMA((4,)),
            DMA((h,)), DMA((h,)), DMA((h,)), DMA((h,)),
            DMA((n, 2)), DMA((n, 2)),
            DMA((G, n, 2)), DMA((G, n, 2)),
            DMA, DMA,
            DMA((h, n // 2)), DMA((h, h // 2, B)),
            DMA((h, h // 2, B)), DMA((h, h // 2, B)),
        ],
        compiler_params=pltpu.CompilerParams(
            collective_id=0, has_side_effects=True, vmem_limit_bytes=63_000_000
        ),
        name="layer",
    )(tokens, gate_weight, up_weight, down_weight)


LANES = 128


def column_layer(
    G, n, B,
    tok, gate, up, down, out,
    X, W, D, Q, S, R, hs, H, acc,
    l_w, l_x, l_d,
    p_send, p_recv, q_send, q_recv, f_send, f_recv, x_send, x_recv,
    t_send, t_recv, c_send, c_recv, d_send, d_recv,
    z_send, z_recv, h_send, h_recv, r_send, r_recv, y_send, y_recv, word,
):
    g, t, b = lax.axis_index("groups"), lax.axis_index("tp"), lax.axis_index("blk")
    h = n // B
    z, y, j, a = t // 2, t % 2, t % h, t // h
    last = n // 2 - 1
    mz = last - z
    inner = z % 2 + a == 1
    outer = z % 2 + a != 1
    own, foreign = b == a, b != a
    rows, depth, wide = tok.shape[0], gate.shape[0], gate.shape[1]
    part, run, half = depth // G, 2 * depth, h // 2 * rows
    chunks = wide // LANES // 2
    other = (g, t, 1 - b)
    beside = (g, flip1(t), b)
    along = flip2(t)
    facing = 2 * mz + y

    near_by = [(g, along, c) for c in range(B)] + [other, beside]
    near_by += [((g + e) % G, t, b) for e in range(1, G)]
    opposite = [(g, facing, c) for c in range(B)]

    @pl.when(inner)
    def _():
        greet(near_by + opposite)

    @pl.when(outer)
    def _():
        greet(near_by)

    def tell(device):
        pl.semaphore_signal(word, inc=1, device_id=device, device_id_type=MESH)

    def hear():
        pl.semaphore_wait(word, 1)

    def remote(src, dst, send, recv, device):
        return pltpu.make_async_remote_copy(
            src_ref=src, dst_ref=dst, send_sem=send, recv_sem=recv,
            device_id=device, device_id_type=MESH,
        )

    def push(*copy):
        remote(*copy).start()

    def got(ref, sem):
        remote(ref, ref, sem, sem, other).wait_recv()

    def sent(ref, sem):
        remote(ref, ref, sem, sem, other).wait_send()

    def lanes(k):
        return pl.ds(pl.multiple_of(k * LANES, LANES), LANES)

    share = pl.ds(pl.multiple_of(g * part, 16), part)

    def landing(k, e):
        return pl.ds(pl.multiple_of(k * depth + e * part, 16), part)

    def w_piece(c, slot, k):
        return W.at[c, landing(slot, g), pl.ds(k * LANES, LANES)]

    def w_share(c, slot, e):
        return W.at[c, landing(slot, e), :]

    def depth_of(row):
        return pl.ds(pl.multiple_of(row * run, LANES), run)

    def x_block(i, k):
        return X.at[
            i // 2, pl.ds(pl.multiple_of(i % 2 * rows, 16), rows),
            pl.ds(pl.multiple_of(k * run, LANES), run),
        ]

    def d_block(i, k):
        return D.at[i, pl.ds(pl.multiple_of(k * LANES, LANES), LANES), :]

    near, beyond, diagonal = flip1(j), flip2(j), flip1(flip2(j))
    z2 = along // 2
    row_there = z2 + b * (last - 2 * z2)
    row_here = z + b * (mz - z)

    def send_across(c):
        for k in range(2):
            push(
                (gate, up)[k].at[share, lanes(y * chunks + c)], w_piece(c, 2 + y, k),
                p_send.at[c, k], p_recv.at[c, k], (g, facing, b),
            )

    def send_beside(c):
        for k in range(2):
            push(
                (gate, up)[k].at[share, lanes((1 - y) * chunks + c)], w_piece(c, y, k),
                q_send.at[c, k], q_recv.at[c, k], beside,
            )

    push(tok.at[:, depth_of(row_there)], x_block(j, b), t_send.at[0], t_recv.at[0], (g, along, b))
    send_beside(0)
    send_beside(1)
    push(tok.at[:, depth_of(row_here)], x_block(j, b), t_send.at[1], t_recv.at[1], beside)
    send_beside(2)

    @pl.when(inner)
    def _():
        send_across(0)
        send_across(1)
        tell((g, facing, b))
        hear()
        tell((g, along, b))

    loads = []
    for k, row in enumerate((z, mz)):
        loads.append(pltpu.make_async_copy(tok.at[:, depth_of(row)], x_block(j, k), l_x.at[k]))
    for c in range(chunks):
        for k in range(2):
            loads.append(pltpu.make_async_copy(
                (gate, up)[k].at[:, lanes(y * chunks + c)],
                W.at[c, pl.ds(pl.multiple_of(y * depth, LANES), depth), pl.ds(k * LANES, LANES)],
                l_w.at[c, k],
            ))
    for i in range(2 * chunks):
        piece = down.at[pl.ds(i * LANES, LANES), :]
        loads.append(pltpu.make_async_copy(piece, d_block(i, b), l_d.at[i]))
        push(piece, d_block(i, b), d_send.at[i], d_recv.at[i], other)
    for load in loads:
        load.start()
    acc[...] = jnp.zeros_like(acc)

    def swap(c, slot, i):
        block = w_share(c, slot, g)
        for e in range(1, G):
            push(block, block, x_send.at[e, c, i], x_recv.at[e, c, i], ((g + e) % G, t, b))

    def from_beside(c):
        for k in range(2):
            got(w_piece(c, 1 - y, k), q_recv.at[c, k])

    def swap_beside(c):
        swap(c, 1 - y, 0)

    def relay(c):
        push(w_share(c, 1 - y, g), w_share(c, 3 - y, g), f_send.at[c], f_recv.at[c], (g, facing, b))

    def from_facing(c):
        for k in range(2):
            got(w_piece(c, 2 + y, k), p_recv.at[c, k])
        swap(c, 2 + y, 1)

    def relayed(c):
        got(w_share(c, 3 - y, g), f_recv.at[c])
        swap(c, 3 - y, 2)

    def pass_tokens(i, k):
        block = x_block(i, b)
        got(block, t_recv.at[k])
        push(block, block, c_send.at[k], c_recv.at[k], other)

    def ready(c):
        for e in range(1, G):
            for i, slot in enumerate((1 - y, 2 + y, 3 - y)):
                got(w_share(c, slot, (g + G - e) % G), x_recv.at[e, c, i])

    def multiply(c, r):
        return jnp.dot(X[r], W[c], preferred_element_type=jnp.float32)

    def keep(c, r):
        Q[c, r] = multiply(c, r)

    def give(c, r):
        S[c, r] = multiply(c, r).astype(S.dtype)
        push(S.at[c, r], R.at[c, r], z_send.at[c, r], z_recv.at[c, r], (g, along, b))

    def h_piece(c, r, k):
        return H.at[y, c, r, :, lanes(k)]

    def finish(c, r):
        got(R.at[c, r], z_recv.at[c, r])
        both = Q[c, r] + R[c, r].astype(jnp.float32)
        hidden = (jax.nn.silu(both[:, :LANES]) * both[:, LANES:]).astype(hs.dtype)
        hs[c, r] = hidden
        block, there = hs.at[c, r], h_piece(c, r, b)
        push(block, there, h_send.at[c, r, 0], h_recv.at[c, r, b], (g, facing, a))
        push(block, there, h_send.at[c, r, 1], h_recv.at[c, r, b], (g, along, a))

        @pl.when(own)
        def _():
            H[y, c, r, :, lanes(b)] = hidden

        @pl.when(foreign)
        def _():
            push(block, there, h_send.at[c, r, 2], h_recv.at[c, r, b], other)

    def onward(c, r):
        push(H.at[y, c, r], H.at[y, c, r], y_send.at[c, r], y_recv.at[c, r], beside)

    def spread_own_inner(c, r):
        got(h_piece(c, r, 1 - b), h_recv.at[c, r, 1 - b])
        onward(c, r)

    def spread_own_outer(c, r):
        for k in range(B):
            got(h_piece(c, r, k), h_recv.at[c, r, k])
        onward(c, r)

    def spread_foreign_inner(c, r):
        for k in range(B):
            got(h_piece(c, r, k), h_recv.at[c, r, k])
        block = H.at[y, c, r]
        push(block, block, r_send.at[c, r], r_recv.at[c, r], (g, along, b))
        onward(c, r)

    def spread_foreign_outer(c, r):
        got(H.at[y, c, r], r_recv.at[c, r])
        onward(c, r)

    def term(c, r):
        got(H.at[1 - y, c, r], y_recv.at[c, r])
        return jnp.dot(H[0, c, r], D[c], preferred_element_type=jnp.float32) + jnp.dot(
            H[1, c, r], D[chunks + c], preferred_element_type=jnp.float32
        )

    def project(c, r):
        acc[r] += term(c, r)

    def deliver(c, r):
        out[pl.ds(pl.multiple_of(r * half, 16), half), :] = (acc[r] + term(c, r)).astype(out.dtype)

    rz = z % 2

    def pass_beyond():
        block = x_block(beyond, b)
        got(block, t_recv.at[0])
        push(block, block, t_send.at[2], t_recv.at[2], beside)
        push(block, block, c_send.at[0], c_recv.at[0], other)
        for c in range(3, chunks):
            send_beside(c)

    def held(i, k):
        got(x_block(i, 1 - b), c_recv.at[k])

    def settle():
        for load in loads:
            load.wait()

    def settle_down():
        for i in range(2 * chunks):
            got(d_block(i, 1 - b), d_recv.at[i])

    def when(role, stage, *args):
        @pl.when(role)
        def _():
            stage(*args)

    halves = (rz, 1 - rz)
    end = chunks - 1

    def tokens_complete():
        pass_tokens(diagonal, 2)
        held(beyond, 0)
        held(diagonal, 2)

    def each(stage, c, order, until=None):
        def body(i, carry):
            r = order[0] + i % 2 * (1 - 2 * order[0])
            stage(c if until is None else c + i // 2, r)
            return carry

        lax.fori_loop(0, 2 if until is None else 2 * (until - c), body, 0)

    @pl.when(inner)
    def _():
        first = (1 - rz, rz)
        from_beside(0)
        relay(0)
        swap_beside(0)
        send_across(2)
        from_facing(0)
        from_facing(1)
        from_beside(1)
        relay(1)
        swap_beside(1)
        relayed(0)
        pass_beyond()
        pass_tokens(near, 1)
        settle()
        held(near, 1)
        ready(0)
        keep(0, rz)
        from_beside(2)
        relay(2)
        tokens_complete()
        from_facing(2)
        keep(0, 1 - rz)
        finish(0, 1 - rz)
        when(own, spread_own_inner, 0, 1 - rz)
        relayed(1)
        from_beside(3)
        swap_beside(2)
        finish(0, rz)
        send_across(3)
        when(own, spread_own_inner, 0, rz)
        settle_down()
        when(foreign, spread_foreign_inner, 0, rz)
        ready(1)
        keep(1, 1 - rz)
        relayed(2)
        finish(1, 1 - rz)
        relay(3)
        when(own, spread_own_inner, 1, 1 - rz)
        when(foreign, spread_foreign_inner, 0, 1 - rz)
        keep(1, rz)
        from_facing(3)
        swap_beside(3)
        ready(2)
        keep(2, 1 - rz)
        finish(1, rz)
        when(own, spread_own_inner, 1, rz)
        when(foreign, spread_foreign_inner, 1, rz)
        keep(2, rz)
        finish(2, 1 - rz)
        relayed(3)
        when(own, spread_own_inner, 2, 1 - rz)
        when(own, each, project, 0, first)
        finish(2, rz)
        when(own, spread_own_inner, 2, rz)
        when(foreign, spread_foreign_inner, 1, 1 - rz)
        when(foreign, spread_foreign_inner, 2, rz)
        ready(3)
        keep(3, 1 - rz)
        when(foreign, spread_foreign_inner, 2, 1 - rz)
        keep(3, rz)

        @pl.when(own)
        def _():
            for r in first:
                finish(3, r)
                spread_own_inner(3, r)
            each(project, 1, first, 3)
            each(deliver, 3, first)

        @pl.when(foreign)
        def _():
            each(finish, 3, first)
            each(spread_foreign_inner, 3, halves)
            each(project, 0, halves, 3)
            each(deliver, 3, halves)

    @pl.when(outer)
    def _():
        far = (1 - rz, rz)
        from_beside(0)
        swap_beside(0)
        hear()
        sent(x_block(j, 0), t_send.at[0])
        send_across(0)
        relay(0)
        send_across(1)
        pass_beyond()
        from_beside(1)
        relay(1)
        send_across(2)
        from_facing(0)
        pass_tokens(near, 1)
        relayed(0)
        swap_beside(1)
        from_beside(2)
        relay(2)
        send_across(3)
        from_facing(1)
        settle()
        held(near, 1)
        ready(0)
        give(0, rz)
        relayed(1)
        from_facing(2)
        tokens_complete()
        give(0, 1 - rz)
        swap_beside(2)
        ready(1)
        give(1, rz)
        from_beside(3)
        relay(3)
        relayed(2)
        give(1, 1 - rz)
        from_facing(3)
        swap_beside(3)
        settle_down()
        when(own, spread_own_outer, 0, rz)
        ready(2)
        each(give, 2, halves)
        when(foreign, spread_foreign_outer, 0, 1 - rz)
        when(own, spread_own_outer, 0, 1 - rz)
        relayed(3)
        ready(3)
        when(own, spread_own_outer, 1, rz)
        when(foreign, spread_foreign_outer, 0, rz)
        give(3, rz)
        when(own, spread_own_outer, 1, 1 - rz)
        give(3, 1 - rz)

        @pl.when(own)
        def _():
            spread_own_outer(2, rz)
            each(project, 0, halves)
            spread_own_outer(2, 1 - rz)
            each(project, 1, halves)
            each(spread_own_outer, 3, halves)
            each(project, 2, halves)
            each(deliver, 3, halves)

        @pl.when(foreign)
        def _():
            for c in (1, 2, 3):
                each(spread_foreign_outer, c, far)
                each(project, c - 1, far)
            each(deliver, 3, far)

    when(inner, sent, x_block(j, 0), t_send.at[0])
    for k in range(3):
        if k:
            sent(x_block(j, 0), t_send.at[k])
        sent(x_block(j, 0), c_send.at[k])
    for i in range(2 * chunks):
        sent(d_block(i, b), d_send.at[i])

    def drain(c, carry):
        for k in range(2):
            sent(w_piece(c, 0, k), p_send.at[c, k])
            sent(w_piece(c, 0, k), q_send.at[c, k])
        sent(w_share(c, 0, g), f_send.at[c])
        for e in range(1, G):
            for i in range(3):
                sent(w_share(c, 0, g), x_send.at[e, c, i])
        for r in range(2):
            sent(H.at[y, c, r], y_send.at[c, r])

            @pl.when(outer)
            def _():
                sent(S.at[c, r], z_send.at[c, r])

            @pl.when(inner)
            def _():
                sent(hs.at[c, r], h_send.at[c, r, 0])
                sent(hs.at[c, r], h_send.at[c, r, 1])

            @pl.when(jnp.logical_and(inner, foreign))
            def _():
                sent(hs.at[c, r], h_send.at[c, r, 2])
                sent(H.at[y, c, r], r_send.at[c, r])

        return carry

    lax.fori_loop(0, chunks, drain, 0)


def column_local(G, n, B, tokens, gate_weight, up_weight, down_weight):
    h = n // B
    rows = tokens.shape[0]
    depth, wide = gate_weight.shape
    columns = down_weight.shape[1]
    chunks = wide // LANES // 2
    half = h // 2 * rows
    dtype = tokens.dtype
    DMA = pltpu.SemaphoreType.DMA
    pair = pltpu.VMEM((chunks, 2, half, 2 * LANES), dtype)
    return pl.pallas_call(
        functools.partial(column_layer, G, n, B),
        out_shape=jax.ShapeDtypeStruct((h * rows, columns), dtype),
        in_specs=[ANY] * 4,
        out_specs=pl.BlockSpec(memory_space=pltpu.VMEM),
        scratch_shapes=[
            pltpu.VMEM((2, half, 4 * depth), dtype),
            pltpu.VMEM((chunks, 4 * depth, 2 * LANES), dtype),
            pltpu.VMEM((2 * chunks, B * LANES, columns), dtype),
            pltpu.VMEM((chunks, 2, half, 2 * LANES), jnp.float32),
            pair, pair,
            pltpu.VMEM((chunks, 2, half, LANES), dtype),
            pltpu.VMEM((2, chunks, 2, half, B * LANES), dtype),
            pltpu.VMEM((2, half, columns), jnp.float32),
            DMA((chunks, 2)), DMA((2,)), DMA((2 * chunks,)),
            DMA((chunks, 2)), DMA((chunks, 2)),
            DMA((chunks, 2)), DMA((chunks, 2)),
            DMA((chunks,)), DMA((chunks,)),
            DMA((G, chunks, 3)), DMA((G, chunks, 3)),
            DMA((3,)), DMA((3,)), DMA((3,)), DMA((3,)),
            DMA((2 * chunks,)), DMA((2 * chunks,)),
            DMA((chunks, 2)), DMA((chunks, 2)),
            DMA((chunks, 2, 3)), DMA((chunks, 2, B)),
            DMA((chunks, 2)), DMA((chunks, 2)),
            DMA((chunks, 2)), DMA((chunks, 2)),
            pltpu.SemaphoreType.REGULAR,
        ],
        compiler_params=pltpu.CompilerParams(
            collective_id=0, has_side_effects=True, vmem_limit_bytes=54_000_000
        ),
        name="layer",
    )(tokens, gate_weight, up_weight, down_weight)


def solution(mesh):
    shape = dict(mesh.shape)
    sizes = shape["groups"], shape["tp"], shape["blk"]
    kernel = column_local if sizes[1:] == (8, 2) else local
    return jax.shard_map(
        functools.partial(kernel, *sizes),
        mesh=mesh,
        in_specs=(P(("groups", "tp"), None), P("tp", "blk"), P("tp", "blk"), P("blk", "tp")),
        out_specs=P(("groups", "blk"), "tp"),
        check_vma=False,
    )
```

```python
import functools

import jax
import jax.numpy as jnp
from jax import lax
from jax.experimental import pallas as pl
from jax.experimental.pallas import tpu as pltpu
from jax.sharding import PartitionSpec as P

MESH = pl.DeviceIdType.MESH
ANY = pl.BlockSpec(memory_space=pl.ANY)


def flip1(i):
    return i + 1 - 2 * (i % 2)


def greet(devices):
    barrier = pltpu.get_barrier_semaphore()
    for device in devices:
        pl.semaphore_signal(barrier, inc=1, device_id=device, device_id_type=MESH)
    pl.semaphore_wait(barrier, len(devices))


def flip2(i):
    return i + 2 - 4 * ((i // 2) % 2)


CUT = 8


def layer(
    G, n, B,
    tok, gate, up, down, out,
    T, W, D, both, mine_h, H, total,
    lsem, tok_send, tok_recv, core_send, core_recv,
    w_send, w_recv, x_send, x_recv, d_send, d_recv,
    h_send, h_recv, f_send, f_recv,
):
    g, t, b = lax.axis_index("groups"), lax.axis_index("tp"), lax.axis_index("blk")
    h = n // B
    a, j = t // h, t % h
    half, pairs = h // 2, n // 2
    p, y = t // 2, t % 2
    other = (g, t, 1 - b)
    across = (g, flip1(t), b)
    R, K = tok.shape
    width = K // B
    depth, units = gate.shape[0], gate.shape[1] // h
    part = depth // G
    mine = pl.ds(pl.multiple_of(b * width, 128), width)
    theirs = pl.ds(pl.multiple_of((1 - b) * width, 128), width)
    square = h == 4
    cut = R * CUT // 16
    upper, lower_rows = pl.ds(0, cut), pl.ds(cut, R - cut)

    greet(
        [(g, (t + d) % n, b) for d in range(1, n)]
        + [(g, 2 * ((p + d) % pairs) + y, 1 - b) for d in range(1, pairs)]
        + [((g + e) % G, t, b) for e in range(1, G)]
        + [other]
    )

    def remote(src, dst, send, recv, device):
        return pltpu.make_async_remote_copy(
            src_ref=src, dst_ref=dst, send_sem=send, recv_sem=recv,
            device_id=device, device_id_type=MESH,
        )

    pending = []

    def push(*copy):
        c = remote(*copy)
        c.start()
        pending.append(c)

    def local(src, dst, sem):
        return pltpu.make_async_copy(src, dst, sem)

    def rows_of(i, s):
        if square:
            i = flip1(i) if s % 2 else i
            return flip2(i) if s // 2 else i
        return (i + h - s) % h

    def token_block(s):
        return T.at[rows_of(j, s), :, mine]

    def w_block(source, first, size, k):
        start = pl.multiple_of(source * depth + first, 16)
        return W.at[pl.ds(start, size), pl.ds(k * units, units)]

    own_columns = pl.ds(pl.multiple_of(j * units, 128), units)
    loads = [
        local(gate.at[:, own_columns], w_block(t, 0, depth, 0), lsem.at[0]),
        local(up.at[:, own_columns], w_block(t, 0, depth, 1), lsem.at[1]),
        local(tok, T.at[j], lsem.at[2]),
        local(down, D.at[b], lsem.at[3]),
    ]

    first = g * part
    rows = pl.ds(pl.multiple_of(first, 16), part)
    order = [d for k in range(1, n // 2) for d in (k, n - k)] + [n // 2]
    for d in order:
        dest = (t + d) % n
        cols = pl.ds(pl.multiple_of((dest % h) * units, 128), units)
        for k in range(2):
            push(
                (gate, up)[k].at[rows, cols], w_block(t, first, part, k),
                w_send.at[d, k], w_recv.at[d, k], (g, dest, b),
            )

    for s in (2, 1) if square else range(1, h):
        dest = rows_of(j, s) if square else (j + s) % h
        push(tok.at[:, mine], T.at[j, :, mine], tok_send.at[s], tok_recv.at[s], (g, a * h + dest, b))
    push(down, D.at[b], d_send, d_recv, other)
    for load in loads:
        load.start()

    for d in order:
        source = (t + n - d) % n
        for k in range(2):
            block = w_block(source, first, part, k)
            remote(block, block, w_send.at[d, k], w_recv.at[d, k], other).wait_recv()
            for e in range(1, G):
                push(block, block, x_send.at[e, d, k], x_recv.at[e, d, k], ((g + e) % G, t, b))
    for load in loads:
        load.wait()
    remote(D.at[1 - b], D.at[1 - b], d_send, d_recv, other).wait_recv()
    total[...] = jnp.zeros_like(total)

    def tokens_arrive(s):
        block = token_block(s)
        if square and s == 3:
            for i, r in ((3, upper), (0, lower_rows)):
                piece = T.at[rows_of(j, s), r, mine]
                remote(piece, piece, tok_send.at[i], tok_recv.at[i], other).wait_recv()
        else:
            remote(block, block, tok_send.at[s], tok_recv.at[s], other).wait_recv()
        if square and s < 3:
            piece = T.at[rows_of(j, s), (upper, lower_rows)[s - 1], mine]
            target = flip2(j) if s == 1 else flip1(j)
            i = 3 if s == 1 else 0
            push(piece, piece, tok_send.at[i], tok_recv.at[i], (g, a * h + target, b))

        push(block, block, core_send.at[s], core_recv.at[s], other)

    def compute(s):
        slot = rows_of(j, s)
        if s > 0:
            block = T.at[slot, :, theirs]
            remote(block, block, core_send.at[s], core_recv.at[s], other).wait_recv()
        tiles = 4 if K % 512 == 0 else 1
        tile = K // tiles
        both[...] = jnp.zeros_like(both)

        def body(i, carry):
            k = pl.ds(pl.multiple_of(i * tile, 128), tile)
            both[...] += jnp.dot(T[slot, :, k], W[k, :], preferred_element_type=jnp.float32)
            return carry

        lax.fori_loop(0, tiles, body, 0)
        hidden = (jax.nn.silu(both[:, :units]) * both[:, units:]).astype(out.dtype)
        mine_h[s] = hidden

        @pl.when(a == b)
        def _():
            H[s, j, b] = hidden

        for d in sorted(range(1, pairs), key=lambda d: min(d, pairs - d)):
            push(
                mine_h.at[s], H.at[s, j, b], h_send.at[s, d], h_recv.at[s, j // 2, b],
                (g, 2 * ((p + d) % pairs) + y, a),
            )

        @pl.when(a != b)
        def _():
            remote(mine_h.at[s], H.at[s, j, b], h_send.at[s, 0], h_recv.at[s, j // 2, b], other).start()

    def pass_on(s):
        for k in range(half):
            for c in range(B):
                block = H.at[s, 2 * k + y, c]

                @pl.when(jnp.logical_not((a == b) & (j // 2 == k) & (c == b)))
                def _():
                    remote(block, block, h_send.at[s, 0], h_recv.at[s, k, c], other).wait_recv()

                push(block, block, f_send.at[s, k, c], f_recv.at[s, k, c], across)

    def lower(s):
        for k in range(half):
            for c in range(B):
                block = H.at[s, 2 * k + 1 - y, c]
                remote(block, block, f_send.at[s, k, c], f_recv.at[s, k, c], across).wait_recv()

        def body(i, carry):
            r = rows_of(i, s)
            term = total[r]
            for c in range(B):
                term += jnp.dot(
                    H[s, i, c], D[c, pl.ds(pl.multiple_of(i * units, 128), units), :],
                    preferred_element_type=jnp.float32,
                )
            total[r] = term
            return carry

        lax.fori_loop(0, h, body, 0)

    for d in order:
        source = (t + n - d) % n
        for e in range(1, G):
            for k in range(2):
                block = w_block(source, ((g + G - e) % G) * part, part, k)
                remote(block, block, x_send.at[e, d, k], x_recv.at[e, d, k], other).wait_recv()

    compute(0)
    for s in range(1, h):
        tokens_arrive(s)
        compute(s)
        pass_on(s - 1)
        if s >= 2:
            lower(s - 2)
    pass_on(h - 1)
    lower(h - 2)
    lower(h - 1)
    for r in range(h):
        out[pl.ds(r * R, R), :] = total[r].astype(out.dtype)

    for c in pending:
        c.wait_send()
    @pl.when(a != b)
    def _():
        for s in range(h):
            remote(mine_h.at[s], mine_h.at[s], h_send.at[s, 0], h_recv.at[s, 0, 0], other).wait_send()


def local(G, n, B, tokens, gate_weight, up_weight, down_weight):
    h = n // B
    R, K = tokens.shape
    depth, wide = gate_weight.shape
    units, columns = wide // h, down_weight.shape[1]
    dtype = tokens.dtype
    DMA = pltpu.SemaphoreType.DMA
    return pl.pallas_call(
        functools.partial(layer, G, n, B),
        out_shape=jax.ShapeDtypeStruct((h * R, columns), dtype),
        in_specs=[ANY] * 4,
        out_specs=pl.BlockSpec(memory_space=pltpu.VMEM),
        scratch_shapes=[
            pltpu.VMEM((h, R, K), dtype),
            pltpu.VMEM((K, 2 * units), dtype),
            pltpu.VMEM((B, wide, columns), dtype),
            pltpu.VMEM((R, 2 * units), jnp.float32),
            pltpu.VMEM((h, R, units), dtype),
            pltpu.VMEM((h, h, B, R, units), dtype),
            pltpu.VMEM((h, R, columns), jnp.float32),
            DMA((4,)),
            DMA((h,)), DMA((h,)), DMA((h,)), DMA((h,)),
            DMA((n, 2)), DMA((n, 2)),
            DMA((G, n, 2)), DMA((G, n, 2)),
            DMA, DMA,
            DMA((h, n // 2)), DMA((h, h // 2, B)),
            DMA((h, h // 2, B)), DMA((h, h // 2, B)),
        ],
        compiler_params=pltpu.CompilerParams(
            collective_id=0, has_side_effects=True, vmem_limit_bytes=63_000_000
        ),
        name="layer",
    )(tokens, gate_weight, up_weight, down_weight)


LANES = 128


def column_layer(
    G, n, B,
    tok, gate, up, down, out,
    X, W, D, Q, S, R, hs, H, acc,
    l_w, l_x, l_d,
    p_send, p_recv, q_send, q_recv, f_send, f_recv, x_send, x_recv,
    t_send, t_recv, c_send, c_recv, d_send, d_recv,
    z_send, z_recv, h_send, h_recv, r_send, r_recv, y_send, y_recv, word,
):
    g, t, b = lax.axis_index("groups"), lax.axis_index("tp"), lax.axis_index("blk")
    h = n // B
    z, y, j, a = t // 2, t % 2, t % h, t // h
    last = n // 2 - 1
    mz = last - z
    inner = z % 2 + a == 1
    outer = z % 2 + a != 1
    own, foreign = b == a, b != a
    rows, depth, wide = tok.shape[0], gate.shape[0], gate.shape[1]
    part, run, half = depth // G, 2 * depth, h // 2 * rows
    chunks = wide // LANES // 2
    other = (g, t, 1 - b)
    beside = (g, flip1(t), b)
    along = flip2(t)
    facing = 2 * mz + y

    near_by = [(g, along, c) for c in range(B)] + [other, beside]
    near_by += [((g + e) % G, t, b) for e in range(1, G)]
    opposite = [(g, facing, c) for c in range(B)]

    @pl.when(inner)
    def _():
        greet(near_by + opposite)

    @pl.when(outer)
    def _():
        greet(near_by)

    def tell(device):
        pl.semaphore_signal(word, inc=1, device_id=device, device_id_type=MESH)

    def hear():
        pl.semaphore_wait(word, 1)

    def remote(src, dst, send, recv, device):
        return pltpu.make_async_remote_copy(
            src_ref=src, dst_ref=dst, send_sem=send, recv_sem=recv,
            device_id=device, device_id_type=MESH,
        )

    def push(*copy):
        remote(*copy).start()

    def got(ref, sem):
        remote(ref, ref, sem, sem, other).wait_recv()

    def sent(ref, sem):
        remote(ref, ref, sem, sem, other).wait_send()

    def lanes(k):
        return pl.ds(pl.multiple_of(k * LANES, LANES), LANES)

    share = pl.ds(pl.multiple_of(g * part, 16), part)

    def landing(k, e):
        return pl.ds(pl.multiple_of(k * depth + e * part, 16), part)

    def w_piece(c, slot, k):
        return W.at[c, landing(slot, g), pl.ds(k * LANES, LANES)]

    def w_share(c, slot, e):
        return W.at[c, landing(slot, e), :]

    def depth_of(row):
        return pl.ds(pl.multiple_of(row * run, LANES), run)

    def x_block(i, k):
        return X.at[
            i // 2, pl.ds(pl.multiple_of(i % 2 * rows, 16), rows),
            pl.ds(pl.multiple_of(k * run, LANES), run),
        ]

    def d_block(i, k):
        return D.at[i, pl.ds(pl.multiple_of(k * LANES, LANES), LANES), :]

    near, beyond, diagonal = flip1(j), flip2(j), flip1(flip2(j))
    z2 = along // 2
    row_there = z2 + b * (last - 2 * z2)
    row_here = z + b * (mz - z)

    def send_across(c):
        for k in range(2):
            push(
                (gate, up)[k].at[share, lanes(y * chunks + c)], w_piece(c, 2 + y, k),
                p_send.at[c, k], p_recv.at[c, k], (g, facing, b),
            )

    def send_beside(c):
        for k in range(2):
            push(
                (gate, up)[k].at[share, lanes((1 - y) * chunks + c)], w_piece(c, y, k),
                q_send.at[c, k], q_recv.at[c, k], beside,
            )

    push(tok.at[:, depth_of(row_there)], x_block(j, b), t_send.at[0], t_recv.at[0], (g, along, b))
    send_beside(0)
    send_beside(1)
    push(tok.at[:, depth_of(row_here)], x_block(j, b), t_send.at[1], t_recv.at[1], beside)
    send_beside(2)

    @pl.when(inner)
    def _():
        send_across(0)
        send_across(1)
        tell((g, facing, b))
        hear()
        tell((g, along, b))

    loads = []
    for k, row in enumerate((z, mz)):
        loads.append(pltpu.make_async_copy(tok.at[:, depth_of(row)], x_block(j, k), l_x.at[k]))
    for c in range(chunks):
        for k in range(2):
            loads.append(pltpu.make_async_copy(
                (gate, up)[k].at[:, lanes(y * chunks + c)],
                W.at[c, pl.ds(pl.multiple_of(y * depth, LANES), depth), pl.ds(k * LANES, LANES)],
                l_w.at[c, k],
            ))
    for i in range(2 * chunks):
        piece = down.at[pl.ds(i * LANES, LANES), :]
        loads.append(pltpu.make_async_copy(piece, d_block(i, b), l_d.at[i]))
        push(piece, d_block(i, b), d_send.at[i], d_recv.at[i], other)
    for load in loads:
        load.start()
    acc[...] = jnp.zeros_like(acc)

    def swap(c, slot, i):
        block = w_share(c, slot, g)
        for e in range(1, G):
            push(block, block, x_send.at[e, c, i], x_recv.at[e, c, i], ((g + e) % G, t, b))

    def from_beside(c):
        for k in range(2):
            got(w_piece(c, 1 - y, k), q_recv.at[c, k])

    def swap_beside(c):
        swap(c, 1 - y, 0)

    def relay(c):
        push(w_share(c, 1 - y, g), w_share(c, 3 - y, g), f_send.at[c], f_recv.at[c], (g, facing, b))

    def from_facing(c):
        for k in range(2):
            got(w_piece(c, 2 + y, k), p_recv.at[c, k])
        swap(c, 2 + y, 1)

    def relayed(c):
        got(w_share(c, 3 - y, g), f_recv.at[c])
        swap(c, 3 - y, 2)

    def pass_tokens(i, k):
        block = x_block(i, b)
        got(block, t_recv.at[k])
        push(block, block, c_send.at[k], c_recv.at[k], other)

    def ready(c):
        for e in range(1, G):
            for i, slot in enumerate((1 - y, 2 + y, 3 - y)):
                got(w_share(c, slot, (g + G - e) % G), x_recv.at[e, c, i])

    def multiply(c, r):
        return jnp.dot(X[r], W[c], preferred_element_type=jnp.float32)

    def keep(c, r):
        Q[c, r] = multiply(c, r)

    def give(c, r):
        S[c, r] = multiply(c, r).astype(S.dtype)
        push(S.at[c, r], R.at[c, r], z_send.at[c, r], z_recv.at[c, r], (g, along, b))

    def h_piece(c, r, k):
        return H.at[y, c, r, :, lanes(k)]

    def finish(c, r):
        got(R.at[c, r], z_recv.at[c, r])
        both = Q[c, r] + R[c, r].astype(jnp.float32)
        hidden = (jax.nn.silu(both[:, :LANES]) * both[:, LANES:]).astype(hs.dtype)
        hs[c, r] = hidden
        block, there = hs.at[c, r], h_piece(c, r, b)
        push(block, there, h_send.at[c, r, 0], h_recv.at[c, r, b], (g, facing, a))
        push(block, there, h_send.at[c, r, 1], h_recv.at[c, r, b], (g, along, a))

        @pl.when(own)
        def _():
            H[y, c, r, :, lanes(b)] = hidden

        @pl.when(foreign)
        def _():
            push(block, there, h_send.at[c, r, 2], h_recv.at[c, r, b], other)

    def onward(c, r):
        push(H.at[y, c, r], H.at[y, c, r], y_send.at[c, r], y_recv.at[c, r], beside)

    def spread_own_inner(c, r):
        got(h_piece(c, r, 1 - b), h_recv.at[c, r, 1 - b])
        onward(c, r)

    def spread_own_outer(c, r):
        for k in range(B):
            got(h_piece(c, r, k), h_recv.at[c, r, k])
        onward(c, r)

    def spread_foreign_inner(c, r):
        for k in range(B):
            got(h_piece(c, r, k), h_recv.at[c, r, k])
        block = H.at[y, c, r]
        push(block, block, r_send.at[c, r], r_recv.at[c, r], (g, along, b))
        onward(c, r)

    def spread_foreign_outer(c, r):
        got(H.at[y, c, r], r_recv.at[c, r])
        onward(c, r)

    def term(c, r):
        got(H.at[1 - y, c, r], y_recv.at[c, r])
        return jnp.dot(H[0, c, r], D[c], preferred_element_type=jnp.float32) + jnp.dot(
            H[1, c, r], D[chunks + c], preferred_element_type=jnp.float32
        )

    def project(c, r):
        acc[r] += term(c, r)

    def deliver(c, r):
        out[pl.ds(pl.multiple_of(r * half, 16), half), :] = (acc[r] + term(c, r)).astype(out.dtype)

    rz = z % 2

    def pass_beyond():
        block = x_block(beyond, b)
        got(block, t_recv.at[0])
        push(block, block, t_send.at[2], t_recv.at[2], beside)
        push(block, block, c_send.at[0], c_recv.at[0], other)
        for c in range(3, chunks):
            send_beside(c)

    def held(i, k):
        got(x_block(i, 1 - b), c_recv.at[k])

    def settle():
        for load in loads:
            load.wait()

    def settle_down():
        for i in range(2 * chunks):
            got(d_block(i, 1 - b), d_recv.at[i])

    def when(role, stage, *args):
        @pl.when(role)
        def _():
            stage(*args)

    halves = (rz, 1 - rz)
    end = chunks - 1

    def tokens_complete():
        pass_tokens(diagonal, 2)
        held(beyond, 0)
        held(diagonal, 2)

    def each(stage, c, order, until=None):
        def body(i, carry):
            r = order[0] + i % 2 * (1 - 2 * order[0])
            stage(c if until is None else c + i // 2, r)
            return carry

        lax.fori_loop(0, 2 if until is None else 2 * (until - c), body, 0)

    @pl.when(inner)
    def _():
        first = (1 - rz, rz)
        from_beside(0)
        relay(0)
        swap_beside(0)
        send_across(2)
        from_facing(0)
        from_facing(1)
        from_beside(1)
        relay(1)
        swap_beside(1)
        relayed(0)
        pass_beyond()
        pass_tokens(near, 1)
        settle()
        held(near, 1)
        ready(0)
        keep(0, rz)
        from_beside(2)
        relay(2)
        tokens_complete()
        from_facing(2)
        keep(0, 1 - rz)
        finish(0, 1 - rz)
        when(own, spread_own_inner, 0, 1 - rz)
        relayed(1)
        from_beside(3)
        swap_beside(2)
        finish(0, rz)
        send_across(3)
        when(own, spread_own_inner, 0, rz)
        settle_down()
        when(foreign, spread_foreign_inner, 0, rz)
        ready(1)
        keep(1, 1 - rz)
        relayed(2)
        finish(1, 1 - rz)
        relay(3)
        when(own, spread_own_inner, 1, 1 - rz)
        when(foreign, spread_foreign_inner, 0, 1 - rz)
        keep(1, rz)
        from_facing(3)
        swap_beside(3)
        ready(2)
        keep(2, 1 - rz)
        finish(1, rz)
        when(own, spread_own_inner, 1, rz)
        when(foreign, spread_foreign_inner, 1, rz)
        keep(2, rz)
        finish(2, 1 - rz)
        relayed(3)
        when(own, spread_own_inner, 2, 1 - rz)
        when(own, each, project, 0, first)
        when(foreign, spread_foreign_inner, 1, 1 - rz)
        finish(2, rz)
        when(own, spread_own_inner, 2, rz)
        when(foreign, spread_foreign_inner, 2, rz)
        ready(3)
        keep(3, 1 - rz)
        when(foreign, spread_foreign_inner, 2, 1 - rz)
        keep(3, rz)

        @pl.when(own)
        def _():
            for r in first:
                finish(3, r)
                spread_own_inner(3, r)
            each(project, 1, first, 3)
            each(deliver, 3, first)

        @pl.when(foreign)
        def _():
            each(finish, 3, first)
            each(spread_foreign_inner, 3, halves)
            each(project, 0, halves, 3)
            each(deliver, 3, halves)

    @pl.when(outer)
    def _():
        far = (1 - rz, rz)
        from_beside(0)
        swap_beside(0)
        hear()
        sent(x_block(j, 0), t_send.at[0])
        send_across(0)
        relay(0)
        send_across(1)
        pass_beyond()
        from_beside(1)
        relay(1)
        send_across(2)
        from_facing(0)
        pass_tokens(near, 1)
        relayed(0)
        swap_beside(1)
        from_beside(2)
        relay(2)
        send_across(3)
        from_facing(1)
        settle()
        held(near, 1)
        ready(0)
        give(0, rz)
        relayed(1)
        from_facing(2)
        tokens_complete()
        give(0, 1 - rz)
        swap_beside(2)
        from_beside(3)
        relay(3)
        ready(1)
        give(1, rz)
        relayed(2)
        give(1, 1 - rz)
        from_facing(3)
        swap_beside(3)
        settle_down()
        ready(2)
        when(own, spread_own_outer, 0, rz)
        each(give, 2, halves)
        when(foreign, spread_foreign_outer, 0, 1 - rz)
        when(own, spread_own_outer, 0, 1 - rz)
        relayed(3)
        ready(3)
        when(own, spread_own_outer, 1, rz)
        when(foreign, spread_foreign_outer, 0, rz)
        give(3, rz)
        when(own, spread_own_outer, 1, 1 - rz)
        give(3, 1 - rz)

        @pl.when(own)
        def _():
            spread_own_outer(2, rz)
            each(project, 0, halves)
            spread_own_outer(2, 1 - rz)
            each(project, 1, halves)
            each(spread_own_outer, 3, halves)
            each(project, 2, halves)
            each(deliver, 3, halves)

        @pl.when(foreign)
        def _():
            for c in (1, 2, 3):
                each(spread_foreign_outer, c, far)
                each(project, c - 1, far)
            each(deliver, 3, far)

    when(inner, sent, x_block(j, 0), t_send.at[0])
    for k in range(3):
        if k:
            sent(x_block(j, 0), t_send.at[k])
        sent(x_block(j, 0), c_send.at[k])
    for i in range(2 * chunks):
        sent(d_block(i, b), d_send.at[i])

    def drain(c, carry):
        for k in range(2):
            sent(w_piece(c, 0, k), p_send.at[c, k])
            sent(w_piece(c, 0, k), q_send.at[c, k])
        sent(w_share(c, 0, g), f_send.at[c])
        for e in range(1, G):
            for i in range(3):
                sent(w_share(c, 0, g), x_send.at[e, c, i])
        for r in range(2):
            sent(H.at[y, c, r], y_send.at[c, r])

            @pl.when(outer)
            def _():
                sent(S.at[c, r], z_send.at[c, r])

            @pl.when(inner)
            def _():
                sent(hs.at[c, r], h_send.at[c, r, 0])
                sent(hs.at[c, r], h_send.at[c, r, 1])

            @pl.when(jnp.logical_and(inner, foreign))
            def _():
                sent(hs.at[c, r], h_send.at[c, r, 2])
                sent(H.at[y, c, r], r_send.at[c, r])

        return carry

    lax.fori_loop(0, chunks, drain, 0)


def column_local(G, n, B, tokens, gate_weight, up_weight, down_weight):
    h = n // B
    rows = tokens.shape[0]
    depth, wide = gate_weight.shape
    columns = down_weight.shape[1]
    chunks = wide // LANES // 2
    half = h // 2 * rows
    dtype = tokens.dtype
    DMA = pltpu.SemaphoreType.DMA
    pair = pltpu.VMEM((chunks, 2, half, 2 * LANES), dtype)
    return pl.pallas_call(
        functools.partial(column_layer, G, n, B),
        out_shape=jax.ShapeDtypeStruct((h * rows, columns), dtype),
        in_specs=[ANY] * 4,
        out_specs=pl.BlockSpec(memory_space=pltpu.VMEM),
        scratch_shapes=[
            pltpu.VMEM((2, half, 4 * depth), dtype),
            pltpu.VMEM((chunks, 4 * depth, 2 * LANES), dtype),
            pltpu.VMEM((2 * chunks, B * LANES, columns), dtype),
            pltpu.VMEM((chunks, 2, half, 2 * LANES), jnp.float32),
            pair, pair,
            pltpu.VMEM((chunks, 2, half, LANES), dtype),
            pltpu.VMEM((2, chunks, 2, half, B * LANES), dtype),
            pltpu.VMEM((2, half, columns), jnp.float32),
            DMA((chunks, 2)), DMA((2,)), DMA((2 * chunks,)),
            DMA((chunks, 2)), DMA((chunks, 2)),
            DMA((chunks, 2)), DMA((chunks, 2)),
            DMA((chunks,)), DMA((chunks,)),
            DMA((G, chunks, 3)), DMA((G, chunks, 3)),
            DMA((3,)), DMA((3,)), DMA((3,)), DMA((3,)),
            DMA((2 * chunks,)), DMA((2 * chunks,)),
            DMA((chunks, 2)), DMA((chunks, 2)),
            DMA((chunks, 2, 3)), DMA((chunks, 2, B)),
            DMA((chunks, 2)), DMA((chunks, 2)),
            DMA((chunks, 2)), DMA((chunks, 2)),
            pltpu.SemaphoreType.REGULAR,
        ],
        compiler_params=pltpu.CompilerParams(
            collective_id=0, has_side_effects=True, vmem_limit_bytes=54_000_000
        ),
        name="layer",
    )(tokens, gate_weight, up_weight, down_weight)


def solution(mesh):
    shape = dict(mesh.shape)
    sizes = shape["groups"], shape["tp"], shape["blk"]
    kernel = column_local if sizes[1:] == (8, 2) else local
    return jax.shard_map(
        functools.partial(kernel, *sizes),
        mesh=mesh,
        in_specs=(P(("groups", "tp"), None), P("tp", "blk"), P("tp", "blk"), P("blk", "tp")),
        out_specs=P(("groups", "blk"), "tp"),
        check_vma=False,
    )
```
